512 devices in a mesh: seq: 64 (over z, y_hi, core), fsdp: 8 (over y_lo, x).
Axes of the slice: x: 4, y: 4 (y_hi: 2, y_lo: 2; y = y_hi * 2 + y_lo), z: 16, core: 2. Of those that a mesh axis runs over, the one named last changes fastest.
Arguments:
- residual: bfloat16 [8, 4096, 1440], P('fsdp', 'seq'), may hold values from -40 to 40
- queries: bfloat16 [8, 4096, 2048], P('fsdp', 'seq'), may hold values from -64 to 64
- key_rows: bfloat16 [8, 4096, 256], P('fsdp', 'seq'), may hold values from -16 to 16
- values: bfloat16 [8, 4096, 256], P('fsdp', 'seq'), may hold values from -1 to 2
- attention_sinks: float32 [32], replicated, may hold values from 0 to 6
- out_weight: bfloat16 [2048, 1440], P('seq', 'fsdp'), may hold values from -0.125 to 0.125
- norm_gain: bfloat16 [1440], replicated, may hold values from 0.25 to 1.75
- router_weight: bfloat16 [1440, 16], replicated, may hold values from -0.15625 to 0.15625
- gate_weight: bfloat16 [1440, 23040], P(None, 'seq'), may hold values from -0.15625 to 0.15625
- up_weight: bfloat16 [1440, 23040], P(None, 'seq'), may hold values from -0.15625 to 0.15625
- down_weight: bfloat16 [23040, 1440], P('seq'), may hold values from -0.15625 to 0.15625
- routing: int32 [8, 4096, 2], P('fsdp', 'seq'), may hold values from 0 to 15, as said below
- span_order: int32 [128], replicated, may hold values from 0 to 127, as said below
Outputs:
- attended: bfloat16 [8, 4096, 1440], P('fsdp', 'seq')
- layer_output: bfloat16 [8, 4096, 1440], P('fsdp', 'seq')
The draws below stay inside these ranges and needn't reach their ends.
Inputs may be any that keep to these rules, and one draw needn't show every extreme that they name: A permutation of 0 to 127; index i of seq holds the rows of spans span_order[2 i] and span_order[2 i + 1], and these two add up to 127. `routing`: in the rows of one device no expert is named more than 12 times; in each prompt one expert is named exactly 12 times in the rows of every device; the 2 experts of a row differ.
All inputs are finite; a program needn't handle non-finite values.
Results may differ from the reference program's by a relative error of at most 0.009.
Values may be sent and summed in bfloat16 or wider, within the bound.
A program may use at most 64 MiB of HBM per device.

```python
import jax
import jax.numpy as jnp
from jax import lax

D = 1440
HEADS = 32
KVH = 4
HD = 64
EXPERTS = 16
FFE = 1440
TOPK = 2
TOK_DEV = 64
HALF = 32
CAP = 12
PROMPTS = 8
TOKENS = 4096
SPANS = 128
UNITS = 360
N_SEQ = 64


def draw_residual(key, part):
    noise_part = jax.random.normal(jax.random.fold_in(key, 7), (PROMPTS, TOKENS, D), jnp.float32)
    return jnp.clip(noise_part, -40.0, 40.0).astype(jnp.bfloat16)


def draw_queries(key, part):
    noise_key = jax.random.fold_in(key, 3)
    drawn = jax.random.normal(noise_key, (PROMPTS, TOKENS, HEADS, HD), jnp.float32)
    return jnp.clip(drawn, -64.0, 64.0).reshape(PROMPTS, TOKENS, HEADS * HD).astype(jnp.bfloat16)


def draw_key_rows(key, part):
    noise_key = jax.random.fold_in(key, 5)
    drawn = jax.random.normal(noise_key, (PROMPTS, TOKENS, KVH, HD), jnp.float32)
    return jnp.clip(drawn, -16.0, 16.0).reshape(PROMPTS, TOKENS, KVH * HD).astype(jnp.bfloat16)


def draw_span_order(key, part):
    pair_index = jax.random.permutation(jax.random.fold_in(key, 21), SPANS // 2).astype(jnp.int32)
    flip_order = jax.random.randint(jax.random.fold_in(key, 22), (SPANS // 2,), 0, 2).astype(jnp.int32)
    first_span = jnp.where(flip_order == 1, SPANS - 1 - pair_index, pair_index)
    return jnp.stack([first_span, SPANS - 1 - first_span], axis=1).reshape(SPANS).astype(jnp.int32)


def route_block(block_key, hot_expert):
    perm_key, order_key, turn_key = jax.random.split(block_key, 3)
    spare_slots = jax.random.permutation(perm_key, (EXPERTS - 1) * CAP)[:TOK_DEV * TOPK - CAP]
    others = (jnp.sort(spare_slots) // CAP).astype(jnp.int32)
    others = others + (others >= hot_expert).astype(jnp.int32)
    listed = jnp.concatenate([jnp.full((CAP,), hot_expert, jnp.int32), others])
    table_rows = listed.reshape(TOPK, TOK_DEV).T
    table_rows = table_rows[jax.random.permutation(order_key, TOK_DEV)]
    turn_by = jax.random.randint(turn_key, (TOK_DEV, 1), 0, TOPK)
    column_order = (jnp.arange(TOPK, dtype=jnp.int32)[None, :] + turn_by) % TOPK
    return jnp.take_along_axis(table_rows, column_order, axis=1).astype(jnp.int32)


def draw_routing(key, part):
    blocks = TOKENS // TOK_DEV
    hot_experts = jax.random.randint(jax.random.fold_in(key, 31), (PROMPTS,), 0, EXPERTS).astype(jnp.int32)
    block_keys = jax.random.split(jax.random.fold_in(key, 32), PROMPTS * blocks)
    hot_each = jnp.repeat(hot_experts, blocks)
    tables = jax.vmap(route_block)(block_keys, hot_each)
    return tables.reshape(PROMPTS, TOKENS, TOPK).astype(jnp.int32)


def steps_of(own_key, dims, pieces, low, top_value):
    def one(axis_at, shards_of):
        steps = jax.random.uniform(jax.random.fold_in(jax.random.fold_in(own_key, 6), axis_at), (shards_of,), jnp.float32, low / len(pieces), top_value / len(pieces))
        return jnp.repeat(jnp.exp(steps), dims[axis_at] // shards_of).reshape((-1,) + (1,) * (len(dims) - axis_at - 1))

    level = one(*pieces[0])
    for cut in pieces[1:]:
        level = level * one(*cut)
    return level


def gaussian(stream_key, dims, scale, bound, shards=(), kind=jnp.bfloat16):
    values = jax.random.normal(stream_key, dims, jnp.float32) * scale
    if len(shards) > 0:
        values = steps_of(stream_key, dims, shards, -0.22, 0.18) * values
    return jnp.clip(values, min=-bound, max=bound).astype(kind)


def setup_inputs(seed: int = 0) -> dict:
    splits = jax.random.split(jax.random.key(seed), 14)
    residual = draw_residual(jax.random.fold_in(splits[13], 71), 0)
    queries = draw_queries(jax.random.fold_in(splits[13], 71), 0)
    key_rows = draw_key_rows(jax.random.fold_in(splits[13], 71), 0)
    values = jnp.clip(-1.0 + 3.0 * jax.random.uniform(splits[3], (PROMPTS, TOKENS, KVH * HD), jnp.float32) ** steps_of(splits[3], (PROMPTS, TOKENS, KVH * HD), ((0, 8), (1, 64)), -0.2, 0.2), -1.0, 2.0).astype(jnp.bfloat16)
    attention_sinks = jnp.clip(jax.random.uniform(splits[4], (HEADS,), jnp.float32, 0.0, 6.0), 0.0, 6.0)
    out_weight = gaussian(splits[5], (HEADS * HD, D), (HEADS * HD) ** -0.5, 0.125, ((0, 64), (1, 8)))
    norm_gain = jnp.clip(1.0 + 0.15 * jax.random.normal(splits[6], (D,), jnp.float32), 0.25, 1.75).astype(jnp.bfloat16)
    router_weight = gaussian(splits[7], (D, EXPERTS), D ** -0.5, 0.15625)
    gate_weight = gaussian(splits[8], (D, EXPERTS * FFE), D ** -0.5, 0.15625, ((1, 64),))
    up_weight = gaussian(splits[9], (D, EXPERTS * FFE), D ** -0.5, 0.15625, ((1, 64),))
    down_weight = gaussian(splits[10], (EXPERTS * FFE, D), FFE ** -0.5, 0.15625, ((0, 64),))
    routing = draw_routing(jax.random.fold_in(splits[13], 71), 0)
    span_order = draw_span_order(jax.random.fold_in(splits[13], 71), 0)
    return dict(residual=residual, queries=queries, key_rows=key_rows, values=values, attention_sinks=attention_sinks, out_weight=out_weight, norm_gain=norm_gain, router_weight=router_weight, gate_weight=gate_weight, up_weight=up_weight, down_weight=down_weight, routing=routing, span_order=span_order)


rope_base = 150000.0
norm_eps = 1e-05
masked_score = -1e+30

def lookup(table_values, lookup_index):
    matches = lookup_index[:, None] == jnp.arange(table_values.shape[0], dtype=jnp.int32)[None, :]
    return lax.optimization_barrier(jnp.sum(jnp.where(matches, table_values[None, :], 0), axis=1)).astype(jnp.int32)

def positions(span_order, row_index):
    device = row_index // TOK_DEV
    within = row_index % TOK_DEV
    span_index = lookup(span_order, 2 * device + within // HALF)
    return span_index * HALF + within % HALF

def rotate(head_values, where_at):
    half_size = head_values.shape[-1] // 2
    frequency = jnp.exp(-jnp.log(rope_base) * jnp.arange(half_size, dtype=jnp.float32) / half_size)
    angles = where_at.astype(jnp.float32)[:, None] * frequency[None, :]
    cosine = jnp.cos(angles)[:, None, :]
    sine_part = jnp.sin(angles)[:, None, :]
    first_half = head_values[..., :half_size]
    second = head_values[..., half_size:]
    return jnp.concatenate([first_half * cosine - second * sine_part, second * cosine + first_half * sine_part], axis=-1)

def slot_of(chosen):
    flattened = chosen.reshape(-1)
    onehot = (flattened[:, None] == jnp.arange(EXPERTS, dtype=jnp.int32)[None, :]).astype(jnp.int32)
    before = jnp.cumsum(onehot, axis=0) - onehot
    return lax.optimization_barrier(jnp.sum(before * onehot, axis=1)).reshape(chosen.shape).astype(jnp.int32)

def reference(residual, queries, key_rows, values, attention_sinks, out_weight, norm_gain, router_weight, gate_weight, up_weight, down_weight, routing, span_order):
    where_at = positions(span_order, jnp.arange(TOKENS, dtype=jnp.int32))
    visible = where_at[None, :] <= where_at[:, None]
    score_scale = HD ** (-0.5)
    group_size = HEADS // KVH

    def attend_prompt(operands):
        query_prompt, key_prompt, value_prompt = operands
        query_rot = rotate(query_prompt.astype(jnp.float32).reshape(TOKENS, HEADS, HD), where_at).astype(jnp.bfloat16)
        key_rot = rotate(key_prompt.astype(jnp.float32).reshape(TOKENS, KVH, HD), where_at).astype(jnp.bfloat16)
        value_heads = value_prompt.reshape(TOKENS, KVH, HD)

        def attend_head(head_index):
            group_index = head_index // group_size
            query_one = lax.dynamic_index_in_dim(query_rot, head_index, 1, keepdims=False).astype(jnp.float32)
            key_one = lax.dynamic_index_in_dim(key_rot, group_index, 1, keepdims=False).astype(jnp.float32)
            value_one = lax.dynamic_index_in_dim(value_heads, group_index, 1, keepdims=False)
            sink_one = lax.dynamic_index_in_dim(attention_sinks, head_index, 0, keepdims=False).astype(jnp.float32)
            scores = jnp.dot(query_one, key_one.T, preferred_element_type=jnp.float32, precision=lax.Precision.HIGHEST) * score_scale
            scores = jnp.where(visible, scores, masked_score)
            row_max = jnp.maximum(lax.optimization_barrier(jnp.max(scores, axis=1)), sink_one)
            weight = jnp.exp(scores - row_max[:, None])
            denominator = lax.optimization_barrier(jnp.sum(weight, axis=1)) + jnp.exp(sink_one - row_max)
            weighted = jnp.dot(weight.astype(jnp.bfloat16), value_one, preferred_element_type=jnp.float32)
            return weighted / denominator[:, None]
        heads_out = lax.map(attend_head, jnp.arange(HEADS, dtype=jnp.int32))
        return jnp.transpose(heads_out, (1, 0, 2)).reshape(TOKENS, HEADS * HD).astype(jnp.bfloat16)
    attention_rows = lax.map(attend_prompt, (queries, key_rows, values))
    attended = jnp.dot(attention_rows.reshape(PROMPTS * TOKENS, HEADS * HD), out_weight, preferred_element_type=jnp.float32).astype(jnp.bfloat16)
    attended = attended.reshape(PROMPTS, TOKENS, D)
    stream = residual.astype(jnp.float32) + attended.astype(jnp.float32)
    normed = (stream * lax.rsqrt(lax.optimization_barrier(jnp.mean(stream * stream, axis=-1, keepdims=True)) + norm_eps) * norm_gain.astype(jnp.float32)).astype(jnp.bfloat16)
    logits = jnp.dot(normed.reshape(PROMPTS * TOKENS, D), router_weight, preferred_element_type=jnp.float32).reshape(PROMPTS, TOKENS, EXPERTS)
    selected = jnp.take_along_axis(logits, routing, axis=-1)
    gates = 1.0 / lax.optimization_barrier(jnp.sum(jnp.exp(selected[..., :, None] - selected[..., None, :]), axis=-2))

    def expert_prompt(operands):
        normed_prompt, chosen_prompt, gates_prompt = operands
        blocks_in = normed_prompt.reshape(N_SEQ, TOK_DEV, D)
        chosen_blocks = chosen_prompt.reshape(N_SEQ, TOK_DEV, TOPK)
        slot_blocks = jax.vmap(slot_of)(chosen_blocks)
        target = chosen_blocks * CAP + slot_blocks

        def dispatch_one(target_block, rows_block):
            mapping = lax.optimization_barrier(jnp.sum((target_block[None, :, :] == jnp.arange(EXPERTS * CAP, dtype=jnp.int32)[:, None, None]).astype(jnp.int32), axis=2))
            return jnp.dot(mapping.astype(jnp.bfloat16), rows_block, preferred_element_type=jnp.float32).astype(jnp.bfloat16)
        buffers = jax.vmap(dispatch_one)(target, blocks_in).reshape(N_SEQ, EXPERTS, CAP, D)

        def run_one(expert_index):
            expert_rows = lax.dynamic_index_in_dim(buffers, expert_index, 1, keepdims=False).reshape(N_SEQ * CAP, D)
            gate_columns = lax.dynamic_slice_in_dim(gate_weight, (expert_index * FFE).astype(jnp.int32), FFE, 1)
            up_columns = lax.dynamic_slice_in_dim(up_weight, (expert_index * FFE).astype(jnp.int32), FFE, 1)
            down_rows = lax.dynamic_slice_in_dim(down_weight, (expert_index * FFE).astype(jnp.int32), FFE, 0)
            gate_values = jnp.dot(expert_rows, gate_columns, preferred_element_type=jnp.float32)
            up_values = jnp.dot(expert_rows, up_columns, preferred_element_type=jnp.float32)
            hidden = (gate_values * jax.nn.sigmoid(1.702 * gate_values) * (up_values + 1.0)).astype(jnp.bfloat16)
            parts = jnp.einsum('rgu,gud->rgd', hidden.reshape(N_SEQ * CAP, FFE // UNITS, UNITS).astype(jnp.float32), down_rows.reshape(FFE // UNITS, UNITS, D).astype(jnp.float32))
            rounded = lax.optimization_barrier(parts.astype(jnp.bfloat16))
            return lax.optimization_barrier(jnp.sum(rounded.astype(jnp.float32), axis=1))
        outputs = lax.map(run_one, jnp.arange(EXPERTS, dtype=jnp.int32)).reshape(EXPERTS * N_SEQ * CAP, D)
        device_index = jnp.arange(N_SEQ, dtype=jnp.int32)[:, None, None]
        flat_index = ((chosen_blocks * N_SEQ + device_index) * CAP + slot_blocks).reshape(-1).astype(jnp.int32)
        chosen_out = jnp.take(outputs, flat_index, axis=0).reshape(TOKENS, TOPK, D)
        return lax.optimization_barrier(jnp.sum(chosen_out * gates_prompt[:, :, None], axis=1))
    expert_mix = lax.map(expert_prompt, (normed, routing, gates))
    layer_output = (stream + expert_mix).astype(jnp.bfloat16)
    return (attended, layer_output)
```

```python
import functools

import jax
import jax.numpy as jnp
from jax import lax
from jax.experimental import pallas as pl
from jax.experimental.pallas import tpu as pltpu
from jax.sharding import PartitionSpec as P

D = 1440
HEADS = 32
KVH = 4
HD = 64
EXPERTS = 16
TOPK = 2
TOK_DEV = 64
HALF = 32
CAP = 12


rope_base = 150000.0
norm_eps = 1e-05
masked_score = -1e30


def swapped(block, axis, distance):
    count = lax.axis_size(axis)
    route = []
    for low in range(count):
        high = low | 1 << distance
        if high != low and high < count:
            route += [(low, high), (high, low)]
    return lax.ppermute(block, axis, route)


def lookup(table_values, lookup_index):
    matches = lookup_index[:, None] == jnp.arange(table_values.shape[0], dtype=jnp.int32)[None, :]
    return jnp.sum(jnp.where(matches, table_values[None, :], 0), axis=1)


def positions(span_order, row_index):
    device = row_index // TOK_DEV
    within = row_index % TOK_DEV
    span_index = lookup(span_order, 2 * device + within // HALF)
    return span_index * HALF + within % HALF


def rotate(head_values, where_at):
    half_size = head_values.shape[-1] // 2
    frequency = jnp.exp(-jnp.log(rope_base) * jnp.arange(half_size, dtype=jnp.float32) / half_size)
    angles = where_at.astype(jnp.float32)[:, None] * frequency[None, :]
    cosine = jnp.cos(angles)[:, None, :]
    sine_part = jnp.sin(angles)[:, None, :]
    first_half = head_values[..., :half_size]
    second = head_values[..., half_size:]
    return jnp.concatenate(
        [first_half * cosine - second * sine_part, second * cosine + first_half * sine_part],
        axis=-1,
    )


def angle_tables(where_at):
    half_size = HD // 2
    frequency = jnp.exp(-jnp.log(rope_base) * jnp.arange(half_size, dtype=jnp.float32) / half_size)
    angles = where_at.astype(jnp.float32)[:, None] * frequency[None, :]
    cosine, sine = jnp.cos(angles), jnp.sin(angles)
    return jnp.tile(cosine, (1, 4)), jnp.tile(jnp.concatenate([-sine, sine], axis=1), (1, 2))


def slot_of(chosen):
    flattened = chosen.reshape(-1)
    onehot = (flattened[:, None] == jnp.arange(EXPERTS, dtype=jnp.int32)[None, :]).astype(jnp.int32)
    before = jnp.cumsum(onehot, axis=0) - onehot
    return jnp.sum(before * onehot, axis=1).reshape(chosen.shape)


def expert_block(flattened, gate_weight, up_weight, down_weight):
    gate_values = jnp.dot(flattened, gate_weight, preferred_element_type=jnp.float32)
    up_values = jnp.dot(flattened, up_weight, preferred_element_type=jnp.float32)
    hidden = (gate_values * jax.nn.sigmoid(1.702 * gate_values) * (up_values + 1.0)).astype(
        jnp.bfloat16
    )
    return jnp.dot(hidden, down_weight, preferred_element_type=jnp.float32).astype(jnp.bfloat16)


MESH_ID = pl.DeviceIdType.MESH
WPAD = 256


def place():
    s = lax.axis_index("seq")
    f = lax.axis_index("fsdp")
    z, hi, c = s // 4, (s // 2) % 2, s % 2
    return z, f % 4, hi * 2 + f // 4, c


def device(z, x, y, c):
    return (z * 4 + (y // 2) * 2 + c, (y % 2) * 4 + x)


def gather_sends(rings):
    half = rings // 2
    kv = 7 + sum((2 * (2 if t < half - 1 else 1) if t < half else 0) for t in range(1, half))
    kv += 4 * (half - 1) + 2
    w = 2 + sum(2 if t < half - 1 else 1 for t in range(1, half)) + 7 * rings
    return kv + w


def gather_kernel(
    rings, kv_ref, w_ref, kv_out, w_out, local_sem, send_sem, kv_sem, a_sem, b_sem, d_sem
):
    half = rings // 2
    z, x, y, c = place()
    hi = y // 2
    s = z * 4 + hi * 2 + c
    turn_x, turn_y = 1 - c, c
    a = x * (1 - c) + y * c
    b = y * (1 - c) + x * c

    def along_z(step):
        return device((z + step + rings) % rings, x, y, c)

    def along_a(step):
        return device(z, (x + step * turn_x + 4) % 4, (y + step * turn_y + 4) % 4, c)

    def along_b(step):
        return device(z, (x + step * turn_y + 4) % 4, (y + step * turn_x + 4) % 4, c)

    other_core = device(z, x, y, 1 - c)
    other_line = device(z, x, (y + 2) % 4, c)
    own_kv = pltpu.make_async_copy(kv_ref, kv_out.at[s], local_sem.at[0])
    own_w = pltpu.make_async_copy(w_ref, w_out.at[c, z, b, a], local_sem.at[1])
    own_kv.start()
    own_w.start()
    greeted = [along_z(1), along_z(-1), other_core, other_line]
    greeted += [along_a(1), along_a(-1), along_b(1), along_b(-1)]
    barrier = pltpu.get_barrier_semaphore()
    for peer in greeted:
        pl.semaphore_signal(barrier, inc=1, device_id=peer, device_id_type=MESH_ID)
    pl.semaphore_wait(barrier, len(greeted))
    own_kv.wait()
    own_w.wait()
    started = []

    def send(ref, recv, peer):
        copy = pltpu.make_async_remote_copy(
            src_ref=ref,
            dst_ref=ref,
            send_sem=send_sem.at[len(started)],
            recv_sem=recv,
            device_id=peer,
            device_id_type=MESH_ID,
        )
        copy.start()
        started.append(copy)

    def arrive(ref, recv):
        pltpu.make_async_remote_copy(
            src_ref=ref,
            dst_ref=ref,
            send_sem=send_sem.at[0],
            recv_sem=recv,
            device_id=other_core,
            device_id_type=MESH_ID,
        ).wait_recv()

    def send_kv(at, peer):
        send(kv_out.at[at], kv_sem.at[at], peer)

    def forwards(t, way, piece):
        if t < half - 1:
            return True
        return t == half - 1 and (piece == 0) == (way == 1)

    def ring_at(t, way):
        return (z - way * t + rings) % rings

    def pieces_at(t):
        if t == 0 or t == half:
            return [(t, 1)]
        return [(t, 1), (t, -1)] if 0 < t < half else []

    def spread_a(t, way):
        zz = ring_at(t, way)
        ref, recv = w_out.at[c, zz, b, a], a_sem.at[zz, a]
        if t > 0:
            arrive(ref, recv)
        if t == 0:
            send(ref, recv, along_z(1))
            send(ref, recv, along_z(-1))
        elif forwards(t, way, 0):
            send(ref, recv, along_z(way))
        send(ref, recv, along_a(1))
        send(ref, recv, along_a(-1))

    def relay_a(t, way):
        zz = ring_at(t, way)
        for step in (-1, 1):
            aa = (a + step + 4) % 4
            arrive(w_out.at[c, zz, b, aa], a_sem.at[zz, aa])
        aa = (a - way + 4) % 4
        send(w_out.at[c, zz, b, aa], a_sem.at[zz, aa], along_a(way))

    def spread_b(t, way):
        zz = ring_at(t, way)
        aa = (a + 2) % 4
        arrive(w_out.at[c, zz, b, aa], a_sem.at[zz, aa])
        for step in (1, -1):
            send(w_out.at[c, zz, b], b_sem.at[zz, b], along_b(step))

    def relay_b(t, way):
        zz = ring_at(t, way)
        for step in (-1, 1):
            bb = (b + step + 4) % 4
            arrive(w_out.at[c, zz, bb], b_sem.at[zz, bb])
        bb = (b - way + 4) % 4
        send(w_out.at[c, zz, bb], b_sem.at[zz, bb], along_b(way))

    def share_w(t, way):
        zz = ring_at(t, way)
        bb = (b + 2) % 4
        arrive(w_out.at[c, zz, bb], b_sem.at[zz, bb])
        send(w_out.at[c, zz], d_sem.at[zz], other_core)

    def step_kv(t):
        if t == 0:
            for peer in (other_line, along_z(1), along_z(-1), other_core):
                send_kv(s, peer)
            across = z * 4 + (1 - hi) * 2 + c
            arrive(kv_out.at[across], kv_sem.at[across])
            for peer in (along_z(1), along_z(-1), other_core):
                send_kv(across, peer)
            return
        for piece in (0, 1):
            for way in (1, -1):
                if t == half and (piece == 0) != (way == 1):
                    continue
                line = hi if piece == 0 else 1 - hi
                at = ring_at(t, way) * 4 + line * 2 + c
                arrive(kv_out.at[at], kv_sem.at[at])
                if forwards(t, way, piece):
                    send_kv(at, along_z(way))
                send_kv(at, other_core)

    for i in range(half + 5):
        for stage, lag in ((spread_a, 0), (step_kv, 0), (relay_a, 1), (spread_b, 2), (relay_b, 3), (share_w, 4)):
            t = i - lag
            if stage is step_kv:
                if t <= half:
                    step_kv(t)
                continue
            for p in pieces_at(t):
                stage(*p)
    for t in range(rings):
        for line in (0, 1):
            at = t * 4 + line * 2 + (1 - c)
            arrive(kv_out.at[at], kv_sem.at[at])
        arrive(w_out.at[1 - c, t], d_sem.at[t])
    assert len(started) <= gather_sends(rings), (len(started), gather_sends(rings))
    for copy in started:
        copy.wait_send()


def gather_all(kv, w, rings):
    rows, width = kv.shape
    w_rows = w.shape[0]
    spec = pl.BlockSpec(memory_space=pltpu.VMEM)
    dma = pltpu.SemaphoreType.DMA
    return pl.pallas_call(
        functools.partial(gather_kernel, rings),
        out_shape=(
            jax.ShapeDtypeStruct((4 * rings, rows, width), kv.dtype),
            jax.ShapeDtypeStruct((2, rings, 4, 4, w_rows, w.shape[1]), w.dtype),
        ),
        in_specs=[spec] * 2,
        out_specs=(spec, spec),
        scratch_shapes=[
            dma((2,)),
            dma((gather_sends(rings),)),
            dma((4 * rings,)),
            dma((rings, 4)),
            dma((rings, 4)),
            dma((rings,)),
        ],
        compiler_params=pltpu.CompilerParams(
            collective_id=0, has_side_effects=True, vmem_limit_bytes=20 * 1024 * 1024
        ),
        name="gather_all",
    )(kv, w)


BLOCK = 256
GROUP = HEADS // KVH


def attention_kernel(
    order_ref, sink_ref, q_ref, cos_ref, sin_ref, kv_ref, w_ref, out_ref, keys, q_sc, max_sc, acc_sc, rows
):
    seq = lax.axis_index("seq")
    spans = order_ref.shape[0]

    def place_span(i, carry):
        at = pl.multiple_of(order_ref[i] * HALF, HALF)
        keys[pl.ds(at, HALF), :] = kv_ref[pl.ds(pl.multiple_of(i * HALF, HALF), HALF), :]
        return carry

    lax.fori_loop(0, spans, place_span, 0, unroll=8)
    lane = lax.broadcasted_iota(jnp.int32, (TOK_DEV, 128), 1)
    low_half = lane % HD < HD // 2
    left = lane < HD
    for tile in range(HEADS // 2):
        raw = q_ref[:, tile * 128 : (tile + 1) * 128].astype(jnp.float32)
        turned = jnp.where(low_half, pltpu.roll(raw, 128 - HD // 2, 1), pltpu.roll(raw, HD // 2, 1))
        rotated = raw * cos_ref[...] + turned * sin_ref[...]
        rotated = rotated.astype(jnp.bfloat16).astype(jnp.float32) * (HD**-0.5)
        swapped_halves = pltpu.roll(rotated, HD, 1)
        for odd in (0, 1):
            head = tile * 2 + odd
            group, member = head // GROUP, head % GROUP
            want_left = group % 2 == 0
            source = rotated if (odd == 0) == want_left else swapped_halves
            kept = jnp.where(left == want_left, source, 0.0).astype(jnp.bfloat16)
            for part in (0, 1):
                q_sc[part, group, member * HALF : (member + 1) * HALF, :] = kept[
                    part * HALF : (part + 1) * HALF
                ]
                max_sc[part, group, member * HALF : (member + 1) * HALF, :] = jnp.full(
                    (HALF, 128), sink_ref[head], jnp.float32
                )
    wide = GROUP * HALF
    acc_left = lax.broadcasted_iota(jnp.int32, (wide, 128), 1) < HD
    for part in (0, 1):
        for group in range(KVH):
            acc_sc[part, group] = jnp.where(acc_left == (group % 2 == 0), 0.0, 1.0)
    v_left = lax.broadcasted_iota(jnp.int32, (BLOCK, 128), 1) < HD
    row_in_span = lax.broadcasted_iota(jnp.int32, (wide, BLOCK), 0) % HALF
    key_in_block = lax.broadcasted_iota(jnp.int32, (wide, BLOCK), 1)

    def unit(part, block, first_query):
        at = pl.multiple_of(block * BLOCK, BLOCK)
        for group in range(KVH):
            tile = group // 2
            key_tile = keys[pl.ds(at, BLOCK), tile * 128 : (tile + 1) * 128]
            value_tile = keys[pl.ds(at, BLOCK), KVH * HD + tile * 128 : KVH * HD + (tile + 1) * 128]
            value_tile = jnp.where(
                v_left == (group % 2 == 0), value_tile, jnp.ones_like(value_tile)
            )
            scores = lax.dot_general(
                q_sc[part, group],
                key_tile,
                (((1,), (1,)), ((), ())),
                preferred_element_type=jnp.float32,
            )
            if first_query is not None:
                scores = jnp.where(
                    key_in_block + at <= row_in_span + first_query, scores, masked_score
                )
            old_max = max_sc[part, group]
            new_max = jnp.maximum(old_max, jnp.max(scores, axis=1, keepdims=True))
            weights = jnp.exp(scores - new_max[:, :1])
            added = jnp.dot(
                weights.astype(jnp.bfloat16), value_tile, preferred_element_type=jnp.float32
            )
            max_sc[part, group] = new_max
            acc_sc[part, group] = acc_sc[part, group] * jnp.exp(old_max - new_max) + added

    per_block = BLOCK // HALF
    for part in (0, 1):
        span = order_ref[2 * seq + part]
        full = span // per_block

        def body(block, carry, part=part):
            unit(part, block, None)
            return carry

        lax.fori_loop(0, full, body, 0)
        unit(part, full, span * HALF)
    for part in (0, 1):
        for group in range(KVH):
            total = acc_sc[part, group]
            divided = total / pltpu.roll(total, HD, 1)
            for pair in range(GROUP // 2):
                one = divided[2 * pair * HALF : (2 * pair + 1) * HALF]
                two = divided[(2 * pair + 1) * HALF : (2 * pair + 2) * HALF]
                if group % 2 == 0:
                    two = pltpu.roll(two, HD, 1)
                else:
                    one = pltpu.roll(one, HD, 1)
                tile = group * (GROUP // 2) + pair
                rows[part * HALF : (part + 1) * HALF, tile * 128 : (tile + 1) * 128] = jnp.where(
                    left[:HALF], one, two
                ).astype(jnp.bfloat16)
    rings = w_ref.shape[1]
    total = jnp.zeros((TOK_DEV, 1536), jnp.float32)
    width = out_ref.shape[1] // 8
    for f in range(8):
        x, low = f % 4, f // 4
        pieces = []
        for z in range(rings):
            for hi in (0, 1):
                y = hi * 2 + low
                pieces += [w_ref[0, z, y, x], w_ref[1, z, x, y]]
        part_out = jnp.dot(
            rows[...], jnp.concatenate(pieces, axis=0), preferred_element_type=jnp.float32
        )
        first = f * width // 128
        shift = f * width - first * 128
        tiles = min(3, 12 - first)
        padded = jnp.concatenate(
            [part_out, jnp.zeros((TOK_DEV, 128), jnp.float32)], axis=1
        )
        if shift:
            padded = pltpu.roll(padded, shift, 1)
        blocks = [total[:, : first * 128], total[:, first * 128 : (first + tiles) * 128] + padded[:, : tiles * 128]]
        if first + tiles < 12:
            blocks.append(total[:, (first + tiles) * 128 :])
        total = jnp.concatenate([k for k in blocks if k.shape[1]], axis=1)
    out_ref[...] = total[:, : out_ref.shape[1]].astype(jnp.bfloat16)


def attend(span_order, sinks, queries, cos, sin, kv_all, w_all):
    spec = pl.BlockSpec(memory_space=pltpu.VMEM)
    smem = pl.BlockSpec(memory_space=pltpu.SMEM)
    wide = GROUP * HALF
    return pl.pallas_call(
        attention_kernel,
        out_shape=jax.ShapeDtypeStruct((TOK_DEV, D), jnp.bfloat16),
        in_specs=[smem, smem] + [spec] * 5,
        out_specs=spec,
        scratch_shapes=[
            pltpu.VMEM(kv_all.shape, jnp.bfloat16),
            pltpu.VMEM((2, KVH, wide, 128), jnp.bfloat16),
            pltpu.VMEM((2, KVH, wide, 128), jnp.float32),
            pltpu.VMEM((2, KVH, wide, 128), jnp.float32),
            pltpu.VMEM((TOK_DEV, HEADS * HD), jnp.bfloat16),
        ],
        compiler_params=pltpu.CompilerParams(vmem_limit_bytes=34 * 1024 * 1024),
        cost_estimate=pl.CostEstimate(flops=4_000_000_000, bytes_accessed=16_000_000, transcendentals=5_000_000),
        name="attend",
    )(span_order, sinks, queries, cos, sin, kv_all, w_all)


def on_device(
    residual,
    queries,
    key_rows,
    values,
    attention_sinks,
    out_weight,
    norm_gain,
    router_weight,
    gate_weight,
    up_weight,
    down_weight,
    routing,
    span_order,
):
    seq_count = lax.axis_size("seq")
    seq_index = lax.axis_index("seq")
    token_count = residual.shape[1]
    query_at = positions(
        span_order, seq_index * token_count + jnp.arange(token_count, dtype=jnp.int32)
    )
    key_rot = rotate(
        key_rows[0].astype(jnp.float32).reshape(token_count, KVH, HD), query_at
    ).astype(jnp.bfloat16)
    kv = jnp.concatenate([key_rot.reshape(token_count, KVH * HD), values[0]], axis=1)
    padded_w = jnp.pad(out_weight, ((0, 0), (0, WPAD - out_weight.shape[1])))
    cos, sin = angle_tables(query_at)
    kv_all, w_all = gather_all(kv, padded_w, seq_count // 4)
    attended = attend(
        span_order,
        attention_sinks,
        queries[0],
        cos,
        sin,
        kv_all.reshape(seq_count * token_count, 2 * KVH * HD),
        w_all,
    )
    stream = residual[0].astype(jnp.float32) + attended.astype(jnp.float32)
    normed = (
        stream
        * lax.rsqrt(jnp.mean(stream * stream, axis=-1, keepdims=True) + norm_eps)
        * norm_gain.astype(jnp.float32)
    ).astype(jnp.bfloat16)
    logits = jnp.dot(normed, router_weight, preferred_element_type=jnp.float32)
    chosen = routing[0]
    matches = chosen[:, :, None] == jnp.arange(EXPERTS, dtype=jnp.int32)[None, None, :]
    chosen_logits = jnp.sum(jnp.where(matches, logits[:, None, :], 0.0), axis=-1)
    gates = 1.0 / jnp.sum(jnp.exp(chosen_logits[:, :, None] - chosen_logits[:, None, :]), axis=1)
    slot_index = slot_of(chosen)
    target = chosen * CAP + slot_index
    dispatch_map = jnp.sum(
        (target[None, :, :] == jnp.arange(EXPERTS * CAP, dtype=jnp.int32)[:, None, None]).astype(
            jnp.int32
        ),
        axis=2,
    )
    buffer = jnp.dot(
        dispatch_map.astype(jnp.bfloat16), normed, preferred_element_type=jnp.float32
    ).astype(jnp.bfloat16)
    copies = seq_count // EXPERTS
    slice_rows = -(-CAP // copies)
    padded = buffer.reshape(EXPERTS, CAP, D).reshape(seq_count, slice_rows, D)
    arrived = lax.all_to_all(padded, "seq", split_axis=0, concat_axis=0, tiled=True)
    bit_count = copies.bit_length() - 1
    gathered = arrived[None]
    for bit in range(bit_count):
        partner = swapped(gathered, "seq", bit)
        upper = seq_index >> bit & 1 == 1
        gathered = jnp.where(
            upper,
            jnp.concatenate([partner, gathered], axis=0),
            jnp.concatenate([gathered, partner], axis=0),
        )
    partial_value = expert_block(
        gathered.reshape(copies * seq_count * slice_rows, D), gate_weight, up_weight, down_weight
    )
    current = partial_value.reshape(copies, seq_count, slice_rows, D).astype(jnp.float32)
    for bit in range(bit_count):
        halves = current.reshape(current.shape[0] // 2, 2, seq_count, slice_rows, D)
        upper = seq_index >> bit & 1 == 1
        kept = jnp.where(upper, halves[:, 1], halves[:, 0])
        given = jnp.where(upper, halves[:, 0], halves[:, 1])
        current = kept + swapped(given.astype(jnp.bfloat16), "seq", bit).astype(given.dtype)
    returned = lax.all_to_all(
        current[0].astype(jnp.bfloat16), "seq", split_axis=0, concat_axis=0, tiled=True
    ).astype(jnp.float32)
    summed = returned.reshape(EXPERTS, copies * slice_rows, D).reshape(EXPERTS * CAP, D)
    chosen_out = jnp.take(summed, target.reshape(-1), axis=0).reshape(token_count, TOPK, D)
    expert_mix = jnp.sum(chosen_out * gates[:, :, None], axis=1)
    layer_output = (stream + expert_mix).astype(jnp.bfloat16)
    return (attended[None], layer_output[None])


def solution(mesh):
    in_specs = (
        P("fsdp", "seq", None),
        P("fsdp", "seq", None),
        P("fsdp", "seq", None),
        P("fsdp", "seq", None),
        P(),
        P("seq", "fsdp"),
        P(),
        P(),
        P(None, "seq"),
        P(None, "seq"),
        P("seq", None),
        P("fsdp", "seq", None),
        P(),
    )
    out_specs = (P("fsdp", "seq", None), P("fsdp", "seq", None))
    return jax.shard_map(
        on_device, mesh=mesh, in_specs=in_specs, out_specs=out_specs, check_vma=False
    )
```

```python
import functools

import jax
import jax.numpy as jnp
from jax import lax
from jax.experimental import pallas as pl
from jax.experimental.pallas import tpu as pltpu
from jax.sharding import PartitionSpec as P

D = 1440
HEADS = 32
KVH = 4
HD = 64
EXPERTS = 16
TOPK = 2
TOK_DEV = 64
HALF = 32
CAP = 12


rope_base = 150000.0
norm_eps = 1e-05
masked_score = -1e30


def lookup(table_values, lookup_index):
    matches = lookup_index[:, None] == jnp.arange(table_values.shape[0], dtype=jnp.int32)[None, :]
    return jnp.sum(jnp.where(matches, table_values[None, :], 0), axis=1)


def positions(span_order, row_index):
    device = row_index // TOK_DEV
    within = row_index % TOK_DEV
    span_index = lookup(span_order, 2 * device + within // HALF)
    return span_index * HALF + within % HALF


def rotate(head_values, where_at):
    half_size = head_values.shape[-1] // 2
    frequency = jnp.exp(-jnp.log(rope_base) * jnp.arange(half_size, dtype=jnp.float32) / half_size)
    angles = where_at.astype(jnp.float32)[:, None] * frequency[None, :]
    cosine = jnp.cos(angles)[:, None, :]
    sine_part = jnp.sin(angles)[:, None, :]
    first_half = head_values[..., :half_size]
    second = head_values[..., half_size:]
    return jnp.concatenate(
        [first_half * cosine - second * sine_part, second * cosine + first_half * sine_part],
        axis=-1,
    )


def angle_tables(where_at):
    half_size = HD // 2
    frequency = jnp.exp(-jnp.log(rope_base) * jnp.arange(half_size, dtype=jnp.float32) / half_size)
    angles = where_at.astype(jnp.float32)[:, None] * frequency[None, :]
    cosine, sine = jnp.cos(angles), jnp.sin(angles)
    return jnp.tile(cosine, (1, 4)), jnp.tile(jnp.concatenate([-sine, sine], axis=1), (1, 2))


MESH_ID = pl.DeviceIdType.MESH
WPAD = 256


def place():
    s = lax.axis_index("seq")
    f = lax.axis_index("fsdp")
    z, hi, c = s // 4, (s // 2) % 2, s % 2
    return z, f % 4, hi * 2 + f // 4, c


def device(z, x, y, c):
    return (z * 4 + (y // 2) * 2 + c, (y % 2) * 4 + x)


def gather_sends(rings):
    half = rings // 2
    kv = 7 + sum((2 * (2 if t < half - 1 else 1) if t < half else 0) for t in range(1, half))
    kv += 4 * (half - 1) + 2
    w = 2 + sum(2 if t < half - 1 else 1 for t in range(1, half)) + 7 * rings
    return kv + w + 3


def gather_kernel(
    rings,
    kv_ref,
    w_ref,
    gate_ref,
    up_ref,
    down_ref,
    kv_out,
    w_out,
    gate_out,
    up_out,
    down_out,
    local_sem,
    send_sem,
    kv_sem,
    a_sem,
    b_sem,
    d_sem,
    e_sem,
):
    half = rings // 2
    z, x, y, c = place()
    hi = y // 2
    s = z * 4 + hi * 2 + c
    turn_x, turn_y = 1 - c, c
    a = x * (1 - c) + y * c
    b = y * (1 - c) + x * c

    def along_z(step):
        return device((z + step + rings) % rings, x, y, c)

    def along_a(step):
        return device(z, (x + step * turn_x + 4) % 4, (y + step * turn_y + 4) % 4, c)

    def along_b(step):
        return device(z, (x + step * turn_y + 4) % 4, (y + step * turn_x + 4) % 4, c)

    other_core = device(z, x, y, 1 - c)
    other_line = device(z, x, (y + 2) % 4, c)
    own_kv = pltpu.make_async_copy(kv_ref, kv_out.at[s], local_sem.at[0])
    own_w = pltpu.make_async_copy(w_ref, w_out.at[c, z, b, a], local_sem.at[1])
    own_kv.start()
    own_w.start()
    greeted = [along_z(1), along_z(-1), other_core, other_line]
    greeted += [along_a(1), along_a(-1), along_b(1), along_b(-1)]
    barrier = pltpu.get_barrier_semaphore()
    for peer in greeted:
        pl.semaphore_signal(barrier, inc=1, device_id=peer, device_id_type=MESH_ID)
    pl.semaphore_wait(barrier, len(greeted))
    own_kv.wait()
    own_w.wait()
    started = []

    def send(ref, recv, peer, landing=None):
        copy = pltpu.make_async_remote_copy(
            src_ref=ref,
            dst_ref=ref if landing is None else landing,
            send_sem=send_sem.at[len(started)],
            recv_sem=recv,
            device_id=peer,
            device_id_type=MESH_ID,
        )
        copy.start()
        started.append(copy)

    def arrive(ref, recv):
        pltpu.make_async_remote_copy(
            src_ref=ref,
            dst_ref=ref,
            send_sem=send_sem.at[0],
            recv_sem=recv,
            device_id=other_core,
            device_id_type=MESH_ID,
        ).wait_recv()

    def send_kv(at, peer):
        send(kv_out.at[at], kv_sem.at[at], peer)

    def forwards(t, way, piece):
        if t < half - 1:
            return True
        return t == half - 1 and (piece == 0) == (way == 1)

    def ring_at(t, way):
        return (z - way * t + rings) % rings

    def pieces_at(t):
        if t == 0 or t == half:
            return [(t, 1)]
        return [(t, 1), (t, -1)] if 0 < t < half else []

    def spread_a(t, way):
        zz = ring_at(t, way)
        ref, recv = w_out.at[c, zz, b, a], a_sem.at[zz, a]
        if t > 0:
            arrive(ref, recv)
        if t == 0:
            send(ref, recv, along_z(1))
            send(ref, recv, along_z(-1))
        elif forwards(t, way, 0):
            send(ref, recv, along_z(way))
        send(ref, recv, along_a(1))
        send(ref, recv, along_a(-1))

    def relay_a(t, way):
        zz = ring_at(t, way)
        for step in (-1, 1):
            aa = (a + step + 4) % 4
            arrive(w_out.at[c, zz, b, aa], a_sem.at[zz, aa])
        aa = (a - way + 4) % 4
        send(w_out.at[c, zz, b, aa], a_sem.at[zz, aa], along_a(way))

    def spread_b(t, way):
        zz = ring_at(t, way)
        aa = (a + 2) % 4
        arrive(w_out.at[c, zz, b, aa], a_sem.at[zz, aa])
        for step in (1, -1):
            send(w_out.at[c, zz, b], b_sem.at[zz, b], along_b(step))

    def relay_b(t, way):
        zz = ring_at(t, way)
        for step in (-1, 1):
            bb = (b + step + 4) % 4
            arrive(w_out.at[c, zz, bb], b_sem.at[zz, bb])
        bb = (b - way + 4) % 4
        send(w_out.at[c, zz, bb], b_sem.at[zz, bb], along_b(way))

    def share_w(t, way):
        zz = ring_at(t, way)
        bb = (b + 2) % 4
        arrive(w_out.at[c, zz, bb], b_sem.at[zz, bb])
        send(w_out.at[c, zz], d_sem.at[zz], other_core)

    def step_kv(t):
        if t == 0:
            for peer in (other_line, along_z(1), along_z(-1), other_core):
                send_kv(s, peer)
            across = z * 4 + (1 - hi) * 2 + c
            arrive(kv_out.at[across], kv_sem.at[across])
            for peer in (along_z(1), along_z(-1), other_core):
                send_kv(across, peer)
            return
        for piece in (0, 1):
            for way in (1, -1):
                if t == half and (piece == 0) != (way == 1):
                    continue
                line = hi if piece == 0 else 1 - hi
                at = ring_at(t, way) * 4 + line * 2 + c
                arrive(kv_out.at[at], kv_sem.at[at])
                if forwards(t, way, piece):
                    send_kv(at, along_z(way))
                send_kv(at, other_core)

    weights = ((gate_ref, gate_out), (up_ref, up_out), (down_ref, down_out))
    for i in range(half + 5):
        for stage, lag in ((spread_a, 0), (step_kv, 0), (relay_a, 1), (spread_b, 2), (relay_b, 3), (share_w, 4)):
            t = i - lag
            if stage is step_kv:
                if t <= half:
                    step_kv(t)
                if t == 2:
                    for n, (mine, landing) in enumerate(weights):
                        send(mine, e_sem.at[n], other_core, landing)
                continue
            for p in pieces_at(t):
                stage(*p)
    for t in range(rings):
        for line in (0, 1):
            at = t * 4 + line * 2 + (1 - c)
            arrive(kv_out.at[at], kv_sem.at[at])
        arrive(w_out.at[1 - c, t], d_sem.at[t])
    for n, (mine, landing) in enumerate(weights):
        arrive(landing, e_sem.at[n])
    assert len(started) <= gather_sends(rings), (len(started), gather_sends(rings))
    for copy in started:
        copy.wait_send()


def gather_all(kv, w, weights, rings):
    rows, width = kv.shape
    w_rows = w.shape[0]
    spec = pl.BlockSpec(memory_space=pltpu.VMEM)
    anywhere = pl.BlockSpec(memory_space=pl.ANY)
    dma = pltpu.SemaphoreType.DMA
    return pl.pallas_call(
        functools.partial(gather_kernel, rings),
        out_shape=(
            jax.ShapeDtypeStruct((4 * rings, rows, width), kv.dtype),
            jax.ShapeDtypeStruct((2, rings, 4, 4, w_rows, w.shape[1]), w.dtype),
            *(jax.ShapeDtypeStruct(v.shape, v.dtype) for v in weights),
        ),
        in_specs=[spec] * 2 + [anywhere] * 3,
        out_specs=(spec, spec) + (anywhere,) * 3,
        scratch_shapes=[
            dma((2,)),
            dma((gather_sends(rings),)),
            dma((4 * rings,)),
            dma((rings, 4)),
            dma((rings, 4)),
            dma((rings,)),
            dma((3,)),
        ],
        compiler_params=pltpu.CompilerParams(
            collective_id=0, has_side_effects=True, vmem_limit_bytes=20 * 1024 * 1024
        ),
        name="gather_all",
    )(kv, w, *weights)


WIDE = 1536
SLOTS = 2 * CAP


def moe_order(blocks):
    order = []
    for i in range(blocks // 2):
        order += [i, blocks - 1 - i]
    return order


def moe_kernel(
    rings,
    chunks,
    normed_ref,
    meta_ref,
    residual_ref,
    attended_ref,
    gate_ref,
    up_ref,
    down_ref,
    gate_other,
    up_other,
    down_other,
    out_ref,
    both,
    both_meta,
    packed,
    arrived,
    partial,
    crossed,
    summed,
    returned,
    mixing,
    give,
    take,
    local_sem,
    send_sem,
    core_sem,
    z_sem,
    y_sem,
    p_sem,
    r_sem,
):
    blocks = rings // 2
    width = residual_ref.shape[1]
    z, x, y, c = place()
    hi = y // 2
    other_core = device(z, x, y, 1 - c)
    other_line = device(z, x, (y + 2) % 4, c)
    middle = blocks // 2
    order = moe_order(blocks)

    def distance(j):
        return 2 * j - blocks + c

    def peer(step):
        return device((z + step + 2 * rings) % rings, x, y, c)

    barrier = pltpu.get_barrier_semaphore()
    for target in (other_core, other_line):
        pl.semaphore_signal(barrier, inc=1, device_id=target, device_id_type=MESH_ID)
    for j in range(blocks):
        if j != middle:
            pl.semaphore_signal(
                barrier, inc=1, device_id=peer(distance(j)), device_id_type=MESH_ID
            )

    @pl.when(c == 1)
    def _():
        pl.semaphore_signal(
            barrier, inc=1, device_id=peer(distance(middle)), device_id_type=MESH_ID
        )

    own_rows = pltpu.make_async_copy(normed_ref, both.at[c], local_sem.at[0])
    own_meta = pltpu.make_async_copy(meta_ref, both_meta.at[c], local_sem.at[1])
    own_rows.start()
    own_meta.start()
    own_rows.wait()
    own_meta.wait()
    pl.semaphore_wait(barrier, blocks + 1 + c)
    started = []
    counter = [0]

    def describe(src, dst, recv, target):
        copy = pltpu.make_async_remote_copy(
            src_ref=src,
            dst_ref=dst,
            send_sem=send_sem.at[counter[0]],
            recv_sem=recv,
            device_id=target,
            device_id_type=MESH_ID,
        )
        counter[0] += 1
        return copy

    def send(src, dst, recv, target):
        copy = describe(src, dst, recv, target)
        copy.start()
        started.append(copy)

    def arrive(ref, recv):
        pltpu.make_async_remote_copy(
            src_ref=ref,
            dst_ref=ref,
            send_sem=send_sem.at[0],
            recv_sem=recv,
            device_id=other_core,
            device_id_type=MESH_ID,
        ).wait_recv()

    conditional = []

    def exchange(j, src, dst, recv, step, sem):
        if j != middle:
            send(src, dst, recv, peer(step))
            return
        copy = describe(src, dst, recv, peer(step))
        conditional.append(copy)

        @pl.when(c == 1)
        def _():
            copy.start()

        @pl.when(c == 0)
        def _():
            kept = pltpu.make_async_copy(src, dst, sem)
            kept.start()
            kept.wait()

    def await_block(j, ref, recv):
        if j != middle:
            arrive(ref, recv)
            return

        @pl.when(c == 1)
        def _():
            arrive(ref, recv)

    send(both.at[c], both.at[c], core_sem.at[0], other_core)
    send(both_meta.at[c], both_meta.at[c], core_sem.at[1], other_core)
    arrive(both.at[1 - c], core_sem.at[0])
    arrive(both_meta.at[1 - c], core_sem.at[1])

    rows = blocks * SLOTS
    at = lax.broadcasted_iota(jnp.int32, (rows, 128), 0)
    token = lax.broadcasted_iota(jnp.int32, (rows, 128), 1)
    block = (at * 2731) >> 16
    rest = at - block * SLOTS
    second = rest >= CAP
    slot = jnp.where(second, rest - CAP, rest)
    expert = (z + 2 * block - blocks + c + 2 * rings) & (rings - 1)
    wanted = jnp.where(second == (token >= TOK_DEV), expert * CAP + slot, -2).astype(jnp.float32)
    meta_lane = lax.broadcasted_iota(jnp.int32, (8, 128), 1)
    meta = jnp.where(meta_lane < TOK_DEV, both_meta[0], both_meta[1])
    first_choice = wanted == meta[0:1]
    second_choice = wanted == meta[1:2]
    picked = jnp.where(first_choice | second_choice, 1.0, 0.0).astype(jnp.bfloat16)
    mixing[...] = jnp.where(first_choice, meta[2:3], 0.0) + jnp.where(
        second_choice, meta[3:4], 0.0
    )
    tokens = jnp.concatenate([both[0], both[1]], axis=0)
    chosen = jnp.dot(picked, tokens, preferred_element_type=jnp.float32)
    packed[...] = chosen.reshape(blocks, 3, 8, chosen.shape[1]).astype(jnp.bfloat16)
    for j in order:
        exchange(j, packed.at[j], arrived.at[hi, j], z_sem.at[j], distance(j), local_sem.at[2])

    def hidden_of(rows_in, gate, up):
        g = jnp.dot(rows_in, gate[...], preferred_element_type=jnp.float32)
        u = jnp.dot(rows_in, up[...], preferred_element_type=jnp.float32)
        return (g * jax.nn.sigmoid(1.702 * g) * (u + 1.0)).astype(jnp.bfloat16)

    def finish(group):
        for j in group:
            arrive(crossed.at[j], p_sem.at[j])
            total = partial[hi, j].astype(jnp.float32) + crossed[j].astype(jnp.float32)
            summed[j] = total.astype(jnp.bfloat16)
            exchange(j, summed.at[j], returned.at[j], r_sem.at[j], -distance(j), local_sem.at[3])

    size = len(order) // chunks
    groups = [order[i * size : (i + 1) * size] for i in range(chunks)]
    before = None
    for group in groups:
        for j in group:
            await_block(j, arrived.at[hi, j], z_sem.at[j])
            send(arrived.at[hi, j], arrived.at[hi, j], y_sem.at[j], other_line)
        for j in group:
            arrive(arrived.at[1 - hi, j], y_sem.at[j])
        pieces = [arrived[line, j].astype(jnp.float32) for line in (0, 1) for j in group]
        rows_in = jnp.concatenate([p.reshape(SLOTS, p.shape[2]) for p in pieces], axis=0)
        rows_in = rows_in.astype(jnp.bfloat16)[:, :width]
        result = jnp.dot(
            hidden_of(rows_in, gate_ref, up_ref), down_ref[...], preferred_element_type=jnp.float32
        )
        result = result + jnp.dot(
            hidden_of(rows_in, gate_other, up_other),
            down_other[...],
            preferred_element_type=jnp.float32,
        )
        for i, (line, j) in enumerate([(line, j) for line in (0, 1) for j in group]):
            one = result[i * SLOTS : (i + 1) * SLOTS].reshape(3, 8, width)
            partial[line, j, :, :, :width] = one.astype(jnp.bfloat16)
        for j in group:
            send(partial.at[1 - hi, j], crossed.at[j], p_sem.at[j], other_line)
        if before is not None:
            finish(before)
        before = group
    finish(before)
    for j in order:
        await_block(j, returned.at[j], r_sem.at[j])
    came_back = jnp.concatenate(
        [returned[j].astype(jnp.float32).reshape(SLOTS, -1) for j in range(blocks)], axis=0
    ).astype(jnp.bfloat16)[:, :width]
    weights = mixing[...]
    coarse = weights.astype(jnp.bfloat16)
    fine = (weights - coarse.astype(jnp.float32)).astype(jnp.bfloat16)
    contract = (((0,), (0,)), ((), ()))
    mixed = lax.dot_general(
        coarse, came_back, contract, preferred_element_type=jnp.float32
    ) + lax.dot_general(fine, came_back, contract, preferred_element_type=jnp.float32)
    upper = c == 1
    give[...] = jnp.where(upper, mixed[:TOK_DEV], mixed[TOK_DEV:])
    send(give, take, core_sem.at[2], other_core)
    stream = residual_ref[...].astype(jnp.float32) + attended_ref[...].astype(jnp.float32)
    kept_rows = stream + jnp.where(upper, mixed[TOK_DEV:], mixed[:TOK_DEV])
    arrive(take, core_sem.at[2])
    out_ref[...] = (kept_rows + take[...]).astype(jnp.bfloat16)
    for copy in started:
        copy.wait_send()

    @pl.when(c == 1)
    def _():
        for copy in conditional:
            copy.wait_send()


def moe(rings, chunks, normed, meta, residual, attended, own, other):
    blocks = rings // 2
    width = residual.shape[1]
    wide = normed.shape[1]
    spec = pl.BlockSpec(memory_space=pltpu.VMEM)
    dma = pltpu.SemaphoreType.DMA
    bf16 = jnp.bfloat16
    return pl.pallas_call(
        functools.partial(moe_kernel, rings, chunks),
        out_shape=jax.ShapeDtypeStruct((TOK_DEV, width), bf16),
        in_specs=[spec] * 10,
        out_specs=spec,
        scratch_shapes=[
            pltpu.VMEM((2, TOK_DEV, wide), bf16),
            pltpu.VMEM((2, 8, 128), jnp.float32),
            pltpu.VMEM((blocks, 3, 8, wide), bf16),
            pltpu.VMEM((2, blocks, 3, 8, wide), bf16),
            pltpu.VMEM((2, blocks, 3, 8, wide), bf16),
            pltpu.VMEM((blocks, 3, 8, wide), bf16),
            pltpu.VMEM((blocks, 3, 8, wide), bf16),
            pltpu.VMEM((blocks, 3, 8, wide), bf16),
            pltpu.VMEM((blocks * SLOTS, 128), jnp.float32),
            pltpu.VMEM((TOK_DEV, width), jnp.float32),
            pltpu.VMEM((TOK_DEV, width), jnp.float32),
            dma((4,)),
            dma((4 * blocks + 4,)),
            dma((3,)),
            dma((blocks,)),
            dma((blocks,)),
            dma((blocks,)),
            dma((blocks,)),
        ],
        compiler_params=pltpu.CompilerParams(
            collective_id=1, has_side_effects=True, vmem_limit_bytes=40 * 1024 * 1024
        ),
        name="moe",
    )(normed, meta, residual, attended, *own, *other)


BLOCK = 256
GROUP = HEADS // KVH


def routing_table(logits, routing):
    core = lax.axis_index("seq") % 2
    expert = lax.broadcasted_iota(jnp.int32, (TOK_DEV, EXPERTS), 1)
    down = lax.broadcasted_iota(jnp.int32, (TOK_DEV, TOK_DEV), 0)
    across = lax.broadcasted_iota(jnp.int32, (TOK_DEV, TOK_DEV), 1)

    def as_row(column):
        return jnp.sum(jnp.where(down == across, column, 0.0), axis=0, keepdims=True)

    columns = [routing[:, k : k + 1] for k in range(TOPK)]
    picked = [
        jnp.sum(jnp.where(expert == column, logits, 0.0), axis=1, keepdims=True)
        for column in columns
    ]
    gates = [1.0 / (1.0 + jnp.exp(picked[1 - k] - picked[k])) for k in range(TOPK)]
    named = [column.astype(jnp.float32) for column in columns]
    lines = []
    for k in range(TOPK):
        row = as_row(named[k])
        earlier = jnp.where(named[0] == row, 1.0, 0.0) + jnp.where(named[1] == row, 1.0, 0.0)
        slot = jnp.sum(jnp.where(down < across, earlier, 0.0), axis=0, keepdims=True)
        lines.append(row * CAP + slot)
    lines += [as_row(gate) for gate in gates]
    lane = lax.broadcasted_iota(jnp.int32, (8, 128), 1)
    line = lax.broadcasted_iota(jnp.int32, (8, 128), 0)
    table = jnp.zeros((8, 128), jnp.float32)
    for k, values in enumerate(lines):
        table = jnp.where(line == k, jnp.concatenate([values, values], axis=1), table)
    return jnp.where((lane >= TOK_DEV) == (core == 1), table, -1.0)


def attention_kernel(
    order_ref,
    sink_ref,
    q_ref,
    cos_ref,
    sin_ref,
    kv_ref,
    w_ref,
    residual_ref,
    gain_ref,
    router_ref,
    routing_ref,
    out_ref,
    normed_ref,
    meta_ref,
    keys,
    q_sc,
    max_sc,
    acc_sc,
    rows,
):
    seq = lax.axis_index("seq")
    spans = order_ref.shape[0]

    def place_span(i, carry):
        at = pl.multiple_of(order_ref[i] * HALF, HALF)
        keys[pl.ds(at, HALF), :] = kv_ref[pl.ds(pl.multiple_of(i * HALF, HALF), HALF), :]
        return carry

    lax.fori_loop(0, spans, place_span, 0, unroll=8)
    lane = lax.broadcasted_iota(jnp.int32, (TOK_DEV, 128), 1)
    low_half = lane % HD < HD // 2
    left = lane < HD
    for tile in range(HEADS // 2):
        raw = q_ref[:, tile * 128 : (tile + 1) * 128].astype(jnp.float32)
        turned = jnp.where(low_half, pltpu.roll(raw, 128 - HD // 2, 1), pltpu.roll(raw, HD // 2, 1))
        rotated = raw * cos_ref[...] + turned * sin_ref[...]
        rotated = rotated.astype(jnp.bfloat16).astype(jnp.float32) * (HD**-0.5)
        swapped_halves = pltpu.roll(rotated, HD, 1)
        for odd in (0, 1):
            head = tile * 2 + odd
            group, member = head // GROUP, head % GROUP
            want_left = group % 2 == 0
            source = rotated if (odd == 0) == want_left else swapped_halves
            kept = jnp.where(left == want_left, source, 0.0).astype(jnp.bfloat16)
            for part in (0, 1):
                q_sc[part, group, member * HALF : (member + 1) * HALF, :] = kept[
                    part * HALF : (part + 1) * HALF
                ]
                max_sc[part, group, member * HALF : (member + 1) * HALF, :] = jnp.full(
                    (HALF, 128), sink_ref[head], jnp.float32
                )
    wide = GROUP * HALF
    acc_left = lax.broadcasted_iota(jnp.int32, (wide, 128), 1) < HD
    for part in (0, 1):
        for group in range(KVH):
            acc_sc[part, group] = jnp.where(acc_left == (group % 2 == 0), 0.0, 1.0)
    v_left = lax.broadcasted_iota(jnp.int32, (BLOCK, 128), 1) < HD
    row_in_span = lax.broadcasted_iota(jnp.int32, (wide, BLOCK), 0) % HALF
    key_in_block = lax.broadcasted_iota(jnp.int32, (wide, BLOCK), 1)

    def unit(part, block, first_query):
        at = pl.multiple_of(block * BLOCK, BLOCK)
        for group in range(KVH):
            tile = group // 2
            key_tile = keys[pl.ds(at, BLOCK), tile * 128 : (tile + 1) * 128]
            value_tile = keys[pl.ds(at, BLOCK), KVH * HD + tile * 128 : KVH * HD + (tile + 1) * 128]
            value_tile = jnp.where(
                v_left == (group % 2 == 0), value_tile, jnp.ones_like(value_tile)
            )
            scores = lax.dot_general(
                q_sc[part, group],
                key_tile,
                (((1,), (1,)), ((), ())),
                preferred_element_type=jnp.float32,
            )
            if first_query is not None:
                scores = jnp.where(
                    key_in_block + at <= row_in_span + first_query, scores, masked_score
                )
            old_max = max_sc[part, group]
            new_max = jnp.maximum(old_max, jnp.max(scores, axis=1, keepdims=True))
            weights = jnp.exp(scores - new_max[:, :1])
            added = jnp.dot(
                weights.astype(jnp.bfloat16), value_tile, preferred_element_type=jnp.float32
            )
            max_sc[part, group] = new_max
            acc_sc[part, group] = acc_sc[part, group] * jnp.exp(old_max - new_max) + added

    per_block = BLOCK // HALF
    for part in (0, 1):
        span = order_ref[2 * seq + part]
        full = span // per_block

        def body(block, carry, part=part):
            unit(part, block, None)
            return carry

        lax.fori_loop(0, full, body, 0)
        unit(part, full, span * HALF)
    for part in (0, 1):
        for group in range(KVH):
            total = acc_sc[part, group]
            divided = total / pltpu.roll(total, HD, 1)
            for pair in range(GROUP // 2):
                one = divided[2 * pair * HALF : (2 * pair + 1) * HALF]
                two = divided[(2 * pair + 1) * HALF : (2 * pair + 2) * HALF]
                if group % 2 == 0:
                    two = pltpu.roll(two, HD, 1)
                else:
                    one = pltpu.roll(one, HD, 1)
                tile = group * (GROUP // 2) + pair
                rows[part * HALF : (part + 1) * HALF, tile * 128 : (tile + 1) * 128] = jnp.where(
                    left[:HALF], one, two
                ).astype(jnp.bfloat16)
    rings = w_ref.shape[1]
    total = jnp.zeros((TOK_DEV, 1536), jnp.float32)
    width = out_ref.shape[1] // 8
    for f in range(8):
        x, low = f % 4, f // 4
        pieces = []
        for z in range(rings):
            for hi in (0, 1):
                y = hi * 2 + low
                pieces += [w_ref[0, z, y, x], w_ref[1, z, x, y]]
        part_out = jnp.dot(
            rows[...], jnp.concatenate(pieces, axis=0), preferred_element_type=jnp.float32
        )
        first = f * width // 128
        shift = f * width - first * 128
        tiles = min(3, 12 - first)
        padded = jnp.concatenate(
            [part_out, jnp.zeros((TOK_DEV, 128), jnp.float32)], axis=1
        )
        if shift:
            padded = pltpu.roll(padded, shift, 1)
        blocks = [total[:, : first * 128], total[:, first * 128 : (first + tiles) * 128] + padded[:, : tiles * 128]]
        if first + tiles < 12:
            blocks.append(total[:, (first + tiles) * 128 :])
        total = jnp.concatenate([k for k in blocks if k.shape[1]], axis=1)
    attended = total[:, :D].astype(jnp.bfloat16)
    out_ref[...] = attended
    stream = residual_ref[...].astype(jnp.float32) + attended.astype(jnp.float32)
    scale = lax.rsqrt(jnp.mean(stream * stream, axis=1, keepdims=True) + norm_eps)
    normed = (stream * scale * gain_ref[...].astype(jnp.float32)).astype(jnp.bfloat16)
    normed_ref[:, 1408:] = jnp.zeros((TOK_DEV, 128), jnp.bfloat16)
    normed_ref[:, :D] = normed
    logits = jnp.dot(normed, router_ref[...], preferred_element_type=jnp.float32)
    meta_ref[...] = routing_table(logits, routing_ref[...])


def attend(span_order, sinks, queries, cos, sin, kv_all, w_all, residual, gain, router, routing):
    spec = pl.BlockSpec(memory_space=pltpu.VMEM)
    smem = pl.BlockSpec(memory_space=pltpu.SMEM)
    wide = GROUP * HALF
    return pl.pallas_call(
        attention_kernel,
        out_shape=(
            jax.ShapeDtypeStruct((TOK_DEV, D), jnp.bfloat16),
            jax.ShapeDtypeStruct((TOK_DEV, WIDE), jnp.bfloat16),
            jax.ShapeDtypeStruct((8, 128), jnp.float32),
        ),
        in_specs=[smem, smem] + [spec] * 9,
        out_specs=(spec, spec, spec),
        scratch_shapes=[
            pltpu.VMEM(kv_all.shape, jnp.bfloat16),
            pltpu.VMEM((2, KVH, wide, 128), jnp.bfloat16),
            pltpu.VMEM((2, KVH, wide, 128), jnp.float32),
            pltpu.VMEM((2, KVH, wide, 128), jnp.float32),
            pltpu.VMEM((TOK_DEV, HEADS * HD), jnp.bfloat16),
        ],
        compiler_params=pltpu.CompilerParams(vmem_limit_bytes=34 * 1024 * 1024),
        cost_estimate=pl.CostEstimate(flops=4_000_000_000, bytes_accessed=16_000_000, transcendentals=5_000_000),
        name="attend",
    )(span_order, sinks, queries, cos, sin, kv_all, w_all, residual, gain, router, routing)


def on_device(
    residual,
    queries,
    key_rows,
    values,
    attention_sinks,
    out_weight,
    norm_gain,
    router_weight,
    gate_weight,
    up_weight,
    down_weight,
    routing,
    span_order,
):
    seq_count = lax.axis_size("seq")
    seq_index = lax.axis_index("seq")
    token_count = residual.shape[1]
    query_at = positions(
        span_order, seq_index * token_count + jnp.arange(token_count, dtype=jnp.int32)
    )
    key_rot = rotate(
        key_rows[0].astype(jnp.float32).reshape(token_count, KVH, HD), query_at
    ).astype(jnp.bfloat16)
    kv = jnp.concatenate([key_rot.reshape(token_count, KVH * HD), values[0]], axis=1)
    padded_w = jnp.pad(out_weight, ((0, 0), (0, WPAD - out_weight.shape[1])))
    cos, sin = angle_tables(query_at)
    own = (gate_weight, up_weight, down_weight)
    rings = seq_count // 4
    kv_all, w_all, *other = gather_all(kv, padded_w, own, rings)
    attended, normed, meta = attend(
        span_order,
        attention_sinks,
        queries[0],
        cos,
        sin,
        kv_all.reshape(seq_count * token_count, 2 * KVH * HD),
        w_all,
        residual[0],
        norm_gain[None, :],
        router_weight,
        routing[0],
    )
    layer_output = moe(rings, 2, normed, meta, residual[0], attended, own, other)
    return (attended[None], layer_output[None])


def solution(mesh):
    in_specs = (
        P("fsdp", "seq", None),
        P("fsdp", "seq", None),
        P("fsdp", "seq", None),
        P("fsdp", "seq", None),
        P(),
        P("seq", "fsdp"),
        P(),
        P(),
        P(None, "seq"),
        P(None, "seq"),
        P("seq", None),
        P("fsdp", "seq", None),
        P(),
    )
    out_specs = (P("fsdp", "seq", None), P("fsdp", "seq", None))
    return jax.shard_map(
        on_device, mesh=mesh, in_specs=in_specs, out_specs=out_specs, check_vma=False
    )
```

```python
import functools

import jax
import jax.numpy as jnp
import numpy as np
from jax import lax
from jax.experimental import pallas as pl
from jax.experimental.pallas import tpu as pltpu
from jax.sharding import PartitionSpec as P

D = 1440
HEADS = 32
KVH = 4
HD = 64
EXPERTS = 16
TOPK = 2
TOK_DEV = 64
HALF = 32
CAP = 12


rope_base = 150000.0
norm_eps = 1e-05
masked_score = -1e30


MESH_ID = pl.DeviceIdType.MESH
def place():
    s = lax.axis_index("seq")
    f = lax.axis_index("fsdp")
    z, hi, c = s // 4, (s // 2) % 2, s % 2
    return z, f % 4, hi * 2 + f // 4, c


def device(z, x, y, c):
    return (z * 4 + (y // 2) * 2 + c, (y % 2) * 4 + x)


PACKED = 48


def angle_tables():
    frequency = np.exp(-np.log(rope_base) * np.arange(HD // 2) / (HD // 2))
    spans = np.arange(2 * TABLE_SPANS)[:, None] * HALF * frequency[None, :]
    steps = np.arange(HALF)[:, None] * frequency[None, :]
    tables = [f(angle) for angle in (spans, steps) for f in (np.cos, np.sin)]
    return [jnp.asarray(np.tile(t, (1, 4)), jnp.float32) for t in tables]


def gather_kernel(
    rings,
    order_ref,
    key_ref,
    value_ref,
    w_ref,
    span_cos,
    span_sin,
    step_cos,
    step_sin,
    gate_ref,
    up_ref,
    down_ref,
    kv_out,
    w_out,
    cos_out,
    sin_out,
    gate_out,
    up_out,
    down_out,
    key_in,
    value_in,
    w_in,
    w_wide,
    table_in,
    step_in,
    local_sem,
    send_sem,
    kv_sem,
    z_sem,
    a_sem,
    b_sem,
    d_sem,
    e_sem,
):
    half = rings // 2
    z, x, y, c = place()
    hi = y // 2
    s = z * 4 + hi * 2 + c
    turn_x, turn_y = 1 - c, c
    a = x * (1 - c) + y * c
    b = y * (1 - c) + x * c

    def along_z(step):
        return device((z + step + rings) % rings, x, y, c)

    def along_a(step):
        return device(z, (x + step * turn_x + 4) % 4, (y + step * turn_y + 4) % 4, c)

    def along_b(step):
        return device(z, (x + step * turn_y + 4) % 4, (y + step * turn_x + 4) % 4, c)

    other_core = device(z, x, y, 1 - c)
    other_line = device(z, x, (y + 2) % 4, c)
    greeted = [along_z(1), along_z(-1), other_core]
    greeted += [along_a(step) for step in (1, -1, 2)] + [along_b(step) for step in (1, -1, 2)]
    barrier = pltpu.get_barrier_semaphore()
    for peer in greeted:
        pl.semaphore_signal(barrier, inc=1, device_id=peer, device_id_type=MESH_ID)
    fetched = [
        pltpu.make_async_copy(src, dst, local_sem.at[n])
        for n, (src, dst) in enumerate(
            (
                (key_ref, key_in),
                (value_ref, value_in),
                (w_ref, w_in),
                (span_cos, table_in.at[0]),
                (span_sin, table_in.at[1]),
                (step_cos, step_in.at[0]),
                (step_sin, step_in.at[1]),
            )
        )
    ]
    for copy in fetched:
        copy.start()
    for copy in fetched:
        copy.wait()
    lane = lax.broadcasted_iota(jnp.int32, (HALF, 128), 1)
    low_half = lane % HD < HD // 2
    for part in (0, 1):
        span = order_ref[2 * s + part]
        far_cos = table_in[0, pl.ds(span, 1), :]
        far_sin = table_in[1, pl.ds(span, 1), :]
        near_cos, near_sin = step_in[0], step_in[1]
        cos = far_cos * near_cos - far_sin * near_sin
        sin = far_sin * near_cos + far_cos * near_sin
        sin = jnp.where(low_half, -sin, sin)
        here = slice(part * HALF, (part + 1) * HALF)
        cos_out[here] = cos
        sin_out[here] = sin
        for tile in range(key_in.shape[1] // 128):
            raw = key_in[here, tile * 128 : (tile + 1) * 128].astype(jnp.float32)
            turned = jnp.where(
                low_half, pltpu.roll(raw, 128 - HD // 2, 1), pltpu.roll(raw, HD // 2, 1)
            )
            kv_out[s, part, :, tile * 128 : (tile + 1) * 128] = (raw * cos + turned * sin).astype(
                jnp.bfloat16
            )
        kv_out[s, part, :, key_in.shape[1] :] = value_in[here]
    w_wide[...] = jnp.zeros_like(w_wide)
    w_wide[:, : w_in.shape[1]] = w_in[...].astype(jnp.float32)
    rest = w_wide[:, 128:]
    w_out[c, z, b, a, :HALF] = w_wide[:, :128].astype(jnp.bfloat16)
    w_out[c, z, b, a, HALF:] = (rest[:16] + pltpu.roll(rest[16:], HD, 1)).astype(jnp.bfloat16)
    pl.semaphore_wait(barrier, len(greeted))
    started = []

    def send(ref, recv, peer, landing=None):
        copy = pltpu.make_async_remote_copy(
            src_ref=ref,
            dst_ref=ref if landing is None else landing,
            send_sem=send_sem.at[len(started)],
            recv_sem=recv,
            device_id=peer,
            device_id_type=MESH_ID,
        )
        copy.start()
        started.append(copy)

    def arrive(ref, recv):
        pltpu.make_async_remote_copy(
            src_ref=ref,
            dst_ref=ref,
            send_sem=send_sem.at[0],
            recv_sem=recv,
            device_id=other_core,
            device_id_type=MESH_ID,
        ).wait_recv()

    def send_kv(at, part, peer):
        send(kv_out.at[at, part], kv_sem.at[at, part], peer)

    def share_kv(at):
        send(kv_out.at[at], kv_sem.at[at, 0], other_core)

    def forwards(t, way, piece):
        if t < half - 1:
            return True
        return t == half - 1 and (piece == 0) == (way == 1)

    def ring_at(t, way):
        return (z - way * t + rings) % rings

    def pieces_at(t):
        if t == 0 or t == half:
            return [(t, 1)]
        return [(t, 1), (t, -1)] if 0 < t < half else []

    def spread_a(t, way):
        zz = ring_at(t, way)
        ref = w_out.at[c, zz, b, a]
        if t > 0:
            arrive(ref, z_sem.at[zz])
        if t == 0:
            send(ref, z_sem.at[zz], along_z(1))
            send(ref, z_sem.at[zz], along_z(-1))
        elif forwards(t, way, 0):
            send(ref, z_sem.at[zz], along_z(way))
        for n, step in enumerate((2, 1, -1)):
            send(ref, a_sem.at[zz, n], along_a(step))

    def spread_b(t, way):
        zz = ring_at(t, way)
        for n, step in enumerate((-2, -1, 1)):
            arrive(w_out.at[c, zz, b, (a + step + 4) % 4], a_sem.at[zz, n])
        for n, step in enumerate((2, 1, -1)):
            send(w_out.at[c, zz, b], b_sem.at[zz, n], along_b(step))

    def share_w(t, way):
        zz = ring_at(t, way)
        for n, step in enumerate((-2, -1, 1)):
            arrive(w_out.at[c, zz, (b + step + 4) % 4], b_sem.at[zz, n])
        send(w_out.at[c, zz], d_sem.at[zz], other_core)

    def step_kv(t):
        if t == 0:
            for part in (0, 1):
                for peer in (other_line, along_z(1), along_z(-1)):
                    send_kv(s, part, peer)
            share_kv(s)
            across = z * 4 + (1 - hi) * 2 + c
            for part in (0, 1):
                arrive(kv_out.at[across, part], kv_sem.at[across, part])
                for peer in (along_z(1), along_z(-1)):
                    send_kv(across, part, peer)
            share_kv(across)
            return
        for piece in (0, 1):
            ways = [way for way in (1, -1) if t < half or (piece == 0) == (way == 1)]
            line = hi if piece == 0 else 1 - hi
            spots = [(way, ring_at(t, way) * 4 + line * 2 + c) for way in ways]
            for part in (0, 1):
                for way, at in spots:
                    arrive(kv_out.at[at, part], kv_sem.at[at, part])
                    if forwards(t, way, piece):
                        send_kv(at, part, along_z(way))
            for way, at in spots:
                share_kv(at)

    weights = ((gate_ref, gate_out), (up_ref, up_out), (down_ref, down_out))
    for i in range(half + LAG_D + 1):
        for p in pieces_at(i):
            spread_a(*p)
        if i <= half:
            step_kv(i)
        if i == 2:
            for n, (mine, landing) in enumerate(weights):
                send(mine, e_sem.at[n], other_core, landing)
        for p in pieces_at(i - LAG_B):
            spread_b(*p)
        for p in pieces_at(i - LAG_D):
            share_w(*p)
    for t in range(rings):
        for line in (0, 1):
            at = t * 4 + line * 2 + (1 - c)
            arrive(kv_out.at[at], kv_sem.at[at, 0])
        arrive(w_out.at[1 - c, t], d_sem.at[t])
    for n, (mine, landing) in enumerate(weights):
        arrive(landing, e_sem.at[n])
    for copy in started:
        copy.wait_send()


LAG_B = 1
LAG_D = 3
TABLE_SPANS = 64


def gather_all(span_order, keys, values, w, weights, rings):
    rows, width = keys.shape
    bf16, f32 = jnp.bfloat16, jnp.float32
    vmem = pl.BlockSpec(memory_space=pltpu.VMEM)
    smem = pl.BlockSpec(memory_space=pltpu.SMEM)
    anywhere = pl.BlockSpec(memory_space=pl.ANY)
    dma = pltpu.SemaphoreType.DMA
    return pl.pallas_call(
        functools.partial(gather_kernel, rings),
        out_shape=(
            jax.ShapeDtypeStruct((4 * rings, 2, rows // 2, 2 * width), bf16),
            jax.ShapeDtypeStruct((2, rings, 4, 4, PACKED, 128), bf16),
            jax.ShapeDtypeStruct((rows, 128), f32),
            jax.ShapeDtypeStruct((rows, 128), f32),
            *(jax.ShapeDtypeStruct(v.shape, v.dtype) for v in weights),
        ),
        in_specs=[smem] + [anywhere] * 10,
        out_specs=(vmem,) * 4 + (anywhere,) * 3,
        scratch_shapes=[
            pltpu.VMEM(keys.shape, bf16),
            pltpu.VMEM(values.shape, bf16),
            pltpu.VMEM(w.shape, bf16),
            pltpu.VMEM((w.shape[0], 256), f32),
            pltpu.VMEM((2, 2 * TABLE_SPANS, 128), f32),
            pltpu.VMEM((2, HALF, 128), f32),
            dma((7,)),
            dma((16 * rings,)),
            dma((4 * rings, 2)),
            dma((rings,)),
            dma((rings, 3)),
            dma((rings, 3)),
            dma((rings,)),
            dma((3,)),
        ],
        compiler_params=pltpu.CompilerParams(
            collective_id=0, has_side_effects=True, vmem_limit_bytes=20 * 1024 * 1024
        ),
        name="gather_all",
    )(span_order, keys, values, w, *angle_tables(), *weights)


WIDE = 1536
SLOTS = 2 * CAP


def routing_table(logits, named, routing_rows):
    core = lax.axis_index("seq") % 2
    expert = lax.broadcasted_iota(jnp.int32, (TOK_DEV, EXPERTS), 1).astype(jnp.float32)
    down = lax.broadcasted_iota(jnp.int32, (TOK_DEV, TOK_DEV), 0)
    across = lax.broadcasted_iota(jnp.int32, (TOK_DEV, TOK_DEV), 1)

    def as_row(column):
        return jnp.sum(jnp.where(down == across, column, 0.0), axis=0, keepdims=True)

    picked = [
        jnp.sum(jnp.where(expert == column, logits, 0.0), axis=1, keepdims=True)
        for column in named
    ]
    gates = [1.0 / (1.0 + jnp.exp(picked[1 - k] - picked[k])) for k in range(TOPK)]
    lines = []
    for k in range(TOPK):
        row = routing_rows[k : k + 1]
        earlier = jnp.where(named[0] == row, 1.0, 0.0) + jnp.where(named[1] == row, 1.0, 0.0)
        slot = jnp.sum(jnp.where(down < across, earlier, 0.0), axis=0, keepdims=True)
        lines.append(row * CAP + slot)
    lines += [as_row(gate) for gate in gates]
    lane = lax.broadcasted_iota(jnp.int32, (8, 128), 1)
    line = lax.broadcasted_iota(jnp.int32, (8, 128), 0)
    table = jnp.zeros((8, 128), jnp.float32)
    for k, values in enumerate(lines):
        table = jnp.where(line == k, jnp.concatenate([values, values], axis=1), table)
    return jnp.where((lane >= TOK_DEV) == (core == 1), table, -1.0)


def project(rows_ref, w_ref):
    rings = w_ref.shape[1]
    rows = rows_ref[...]
    feature = lax.broadcasted_iota(jnp.int32, rows.shape, 1)
    first = feature % HALF < 16
    stacked = jnp.concatenate(
        [jnp.where(first, rows, 0).astype(rows.dtype), jnp.where(first, 0, rows).astype(rows.dtype)],
        axis=0,
    )
    lane = lax.broadcasted_iota(jnp.int32, (TOK_DEV, 128), 1)
    width = D // 8
    total = jnp.zeros((TOK_DEV, WIDE), jnp.float32)
    for f in range(8):
        x, low = f % 4, f // 4
        pieces = []
        for z in range(rings):
            for hi in (0, 1):
                y = hi * 2 + low
                pieces += [w_ref.at[0, z, y, x], w_ref.at[1, z, x, y]]
        main = jnp.concatenate([p[:HALF] for p in pieces], axis=0)
        rest = jnp.concatenate([p[HALF:] for p in pieces for _ in (0, 1)], axis=0)
        head = jnp.dot(rows, main, preferred_element_type=jnp.float32)
        tail = jnp.dot(stacked, rest, preferred_element_type=jnp.float32)
        tail = jnp.where(lane < HD, tail[:TOK_DEV] + pltpu.roll(tail[TOK_DEV:], HD, 1), 0.0)
        begin = f * width // 128
        shift = f * width - begin * 128
        tiles = min(3, 12 - begin)
        padded = jnp.concatenate([head, tail, jnp.zeros((TOK_DEV, 128), jnp.float32)], axis=1)
        if shift:
            padded = pltpu.roll(padded, shift, 1)
        span = slice(begin * 128, (begin + tiles) * 128)
        blocks = [total[:, : span.start], total[:, span] + padded[:, : tiles * 128]]
        blocks.append(total[:, span.stop :])
        total = jnp.concatenate([k for k in blocks if k.shape[1]], axis=1)
    return total[:, :D].astype(jnp.bfloat16)


def moe_order(blocks):
    order = []
    for i in range(blocks // 2):
        order += [i, blocks - 1 - i]
    return order


def moe_kernel(
    rings,
    chunks,
    project_rows,
    rows_ref,
    w_ref,
    residual_ref,
    gain_ref,
    router_ref,
    routing_ref,
    gate_ref,
    up_ref,
    down_ref,
    gate_other,
    up_other,
    down_other,
    attended_ref,
    out_ref,
    both,
    both_meta,
    packed,
    arrived,
    partial,
    crossed,
    summed,
    returned,
    mixing,
    give,
    take,
    local_sem,
    send_sem,
    core_sem,
    z_sem,
    y_sem,
    p_sem,
    r_sem,
):
    blocks = rings // 2
    width = residual_ref.shape[1]
    z, x, y, c = place()
    hi = y // 2
    other_core = device(z, x, y, 1 - c)
    other_line = device(z, x, (y + 2) % 4, c)
    middle = blocks // 2
    order = moe_order(blocks)

    def distance(j):
        return 2 * j - blocks + c

    def peer(step):
        return device((z + step + 2 * rings) % rings, x, y, c)

    barrier = pltpu.get_barrier_semaphore()
    for target in (other_core, other_line):
        pl.semaphore_signal(barrier, inc=1, device_id=target, device_id_type=MESH_ID)
    for j in range(blocks):
        if j != middle:
            pl.semaphore_signal(
                barrier, inc=1, device_id=peer(distance(j)), device_id_type=MESH_ID
            )

    @pl.when(c == 1)
    def _():
        pl.semaphore_signal(
            barrier, inc=1, device_id=peer(distance(middle)), device_id_type=MESH_ID
        )

    attended = project_rows(rows_ref, w_ref)
    attended_ref[...] = attended
    stream = residual_ref[...].astype(jnp.float32) + attended.astype(jnp.float32)
    scale = lax.rsqrt(jnp.mean(stream * stream, axis=1, keepdims=True) + norm_eps)
    normed = (stream * scale * gain_ref[...].astype(jnp.float32)).astype(jnp.bfloat16)
    both[c, :, width - width % 128 :] = jnp.zeros((TOK_DEV, 128), jnp.bfloat16)
    both[c, :, :width] = normed
    logits = lax.dot_general(
        normed, router_ref[...], (((1,), (1,)), ((), ())), preferred_element_type=jnp.float32
    )
    routed = routing_ref[...].astype(jnp.float32)
    down = lax.broadcasted_iota(jnp.int32, (TOK_DEV, TOK_DEV), 0)
    across = lax.broadcasted_iota(jnp.int32, (TOK_DEV, TOK_DEV), 1)
    named = [
        jnp.sum(jnp.where(down == across, routed[k : k + 1], 0.0), axis=1, keepdims=True)
        for k in range(TOPK)
    ]
    both_meta[c] = routing_table(logits, named, routed)
    pl.semaphore_wait(barrier, blocks + 1 + c)
    started = []
    counter = [0]

    def describe(src, dst, recv, target):
        copy = pltpu.make_async_remote_copy(
            src_ref=src,
            dst_ref=dst,
            send_sem=send_sem.at[counter[0]],
            recv_sem=recv,
            device_id=target,
            device_id_type=MESH_ID,
        )
        counter[0] += 1
        return copy

    def send(src, dst, recv, target):
        copy = describe(src, dst, recv, target)
        copy.start()
        started.append(copy)

    def arrive(ref, recv):
        pltpu.make_async_remote_copy(
            src_ref=ref,
            dst_ref=ref,
            send_sem=send_sem.at[0],
            recv_sem=recv,
            device_id=other_core,
            device_id_type=MESH_ID,
        ).wait_recv()

    conditional = []

    def exchange(j, src, dst, recv, step, sem):
        if j != middle:
            send(src, dst, recv, peer(step))
            return
        copy = describe(src, dst, recv, peer(step))
        conditional.append(copy)

        @pl.when(c == 1)
        def _():
            copy.start()

        @pl.when(c == 0)
        def _():
            kept = pltpu.make_async_copy(src, dst, sem)
            kept.start()
            kept.wait()

    def await_block(j, ref, recv):
        if j != middle:
            arrive(ref, recv)
            return

        @pl.when(c == 1)
        def _():
            arrive(ref, recv)

    send(both.at[c], both.at[c], core_sem.at[0], other_core)
    send(both_meta.at[c], both_meta.at[c], core_sem.at[1], other_core)
    arrive(both.at[1 - c], core_sem.at[0])
    arrive(both_meta.at[1 - c], core_sem.at[1])

    rows = blocks * SLOTS
    at = lax.broadcasted_iota(jnp.int32, (rows, 128), 0)
    token = lax.broadcasted_iota(jnp.int32, (rows, 128), 1)
    block = (at * 2731) >> 16
    rest = at - block * SLOTS
    second = rest >= CAP
    slot = jnp.where(second, rest - CAP, rest)
    expert = (z + 2 * block - blocks + c + 2 * rings) & (rings - 1)
    wanted = jnp.where(second == (token >= TOK_DEV), expert * CAP + slot, -2).astype(jnp.float32)
    meta_lane = lax.broadcasted_iota(jnp.int32, (8, 128), 1)
    meta = jnp.where(meta_lane < TOK_DEV, both_meta[0], both_meta[1])
    first_choice = wanted == meta[0:1]
    second_choice = wanted == meta[1:2]
    picked = jnp.where(first_choice | second_choice, 1.0, 0.0).astype(jnp.bfloat16)
    mixing[...] = jnp.where(first_choice, meta[2:3], 0.0) + jnp.where(
        second_choice, meta[3:4], 0.0
    )
    tokens = jnp.concatenate([both[0], both[1]], axis=0)
    chosen = jnp.dot(picked, tokens, preferred_element_type=jnp.float32)
    packed[...] = chosen.reshape(blocks, 3, 8, chosen.shape[1]).astype(jnp.bfloat16)
    for j in order:
        exchange(j, packed.at[j], arrived.at[hi, j], z_sem.at[j], distance(j), local_sem.at[2])

    def hidden_of(rows_in, gate, up):
        g = jnp.dot(rows_in, gate[...], preferred_element_type=jnp.float32)
        u = jnp.dot(rows_in, up[...], preferred_element_type=jnp.float32)
        return (g * jax.nn.sigmoid(1.702 * g) * (u + 1.0)).astype(jnp.bfloat16)

    def finish(group):
        for j in group:
            arrive(crossed.at[j], p_sem.at[j])
            total = partial[hi, j].astype(jnp.float32) + crossed[j].astype(jnp.float32)
            summed[j] = total.astype(jnp.bfloat16)
            exchange(j, summed.at[j], returned.at[j], r_sem.at[j], -distance(j), local_sem.at[3])

    size = len(order) // chunks
    groups = [order[i * size : (i + 1) * size] for i in range(chunks)]
    before = None
    for group in groups:
        for j in group:
            await_block(j, arrived.at[hi, j], z_sem.at[j])
            send(arrived.at[hi, j], arrived.at[hi, j], y_sem.at[j], other_line)
        for j in group:
            arrive(arrived.at[1 - hi, j], y_sem.at[j])
        pieces = [arrived[line, j].astype(jnp.float32) for line in (0, 1) for j in group]
        rows_in = jnp.concatenate([p.reshape(SLOTS, p.shape[2]) for p in pieces], axis=0)
        rows_in = rows_in.astype(jnp.bfloat16)[:, :width]
        result = jnp.dot(
            hidden_of(rows_in, gate_ref, up_ref), down_ref[...], preferred_element_type=jnp.float32
        )
        result = result + jnp.dot(
            hidden_of(rows_in, gate_other, up_other),
            down_other[...],
            preferred_element_type=jnp.float32,
        )
        for i, (line, j) in enumerate([(line, j) for line in (0, 1) for j in group]):
            one = result[i * SLOTS : (i + 1) * SLOTS].reshape(3, 8, width)
            partial[line, j, :, :, :width] = one.astype(jnp.bfloat16)
        for j in group:
            send(partial.at[1 - hi, j], crossed.at[j], p_sem.at[j], other_line)
        if before is not None:
            finish(before)
        before = group
    finish(before)
    for j in order:
        await_block(j, returned.at[j], r_sem.at[j])
    came_back = jnp.concatenate(
        [returned[j].astype(jnp.float32).reshape(SLOTS, -1) for j in range(blocks)], axis=0
    ).astype(jnp.bfloat16)[:, :width]
    weights = mixing[...]
    coarse = weights.astype(jnp.bfloat16)
    fine = (weights - coarse.astype(jnp.float32)).astype(jnp.bfloat16)
    contract = (((0,), (0,)), ((), ()))
    mixed = lax.dot_general(
        coarse, came_back, contract, preferred_element_type=jnp.float32
    ) + lax.dot_general(fine, came_back, contract, preferred_element_type=jnp.float32)
    upper = c == 1
    give[...] = jnp.where(upper, mixed[:TOK_DEV], mixed[TOK_DEV:])
    send(give, take, core_sem.at[2], other_core)
    stream = residual_ref[...].astype(jnp.float32) + attended_ref[...].astype(jnp.float32)
    kept_rows = stream + jnp.where(upper, mixed[TOK_DEV:], mixed[:TOK_DEV])
    arrive(take, core_sem.at[2])
    out_ref[...] = (kept_rows + take[...]).astype(jnp.bfloat16)
    for copy in started:
        copy.wait_send()

    @pl.when(c == 1)
    def _():
        for copy in conditional:
            copy.wait_send()


def moe(rings, chunks, rows, w_all, residual, gain, router, routing, own, other, wide=WIDE, project_rows=project):
    blocks = rings // 2
    width = residual.shape[1]
    spec = pl.BlockSpec(memory_space=pltpu.VMEM)
    dma = pltpu.SemaphoreType.DMA
    bf16 = jnp.bfloat16
    return pl.pallas_call(
        functools.partial(moe_kernel, rings, chunks, project_rows),
        out_shape=(jax.ShapeDtypeStruct((TOK_DEV, width), bf16),) * 2,
        in_specs=[spec] * 12,
        out_specs=(spec, spec),
        scratch_shapes=[
            pltpu.VMEM((2, TOK_DEV, wide), bf16),
            pltpu.VMEM((2, 8, 128), jnp.float32),
            pltpu.VMEM((blocks, 3, 8, wide), bf16),
            pltpu.VMEM((2, blocks, 3, 8, wide), bf16),
            pltpu.VMEM((2, blocks, 3, 8, wide), bf16),
            pltpu.VMEM((blocks, 3, 8, wide), bf16),
            pltpu.VMEM((blocks, 3, 8, wide), bf16),
            pltpu.VMEM((blocks, 3, 8, wide), bf16),
            pltpu.VMEM((blocks * SLOTS, 128), jnp.float32),
            pltpu.VMEM((TOK_DEV, width), jnp.float32),
            pltpu.VMEM((TOK_DEV, width), jnp.float32),
            dma((4,)),
            dma((4 * blocks + 4,)),
            dma((3,)),
            dma((blocks,)),
            dma((blocks,)),
            dma((blocks,)),
            dma((blocks,)),
        ],
        compiler_params=pltpu.CompilerParams(
            collective_id=1, has_side_effects=True, vmem_limit_bytes=40 * 1024 * 1024
        ),
        name="moe",
    )(rows, w_all, residual, gain, router, routing, *own, *other)


BLOCK = 1024
GROUP = HEADS // KVH


def attention_kernel(
    order_ref,
    sink_ref,
    q_ref,
    cos_ref,
    sin_ref,
    kv_ref,
    rows,
    keys,
    q_sc,
    max_sc,
    acc_sc,
):
    seq = lax.axis_index("seq")
    spans = order_ref.shape[0]

    def place_span(i, carry):
        at = pl.multiple_of(order_ref[i] * HALF, HALF)
        keys[pl.ds(at, HALF), :] = kv_ref[pl.ds(pl.multiple_of(i * HALF, HALF), HALF), :]
        return carry

    lax.fori_loop(0, spans, place_span, 0, unroll=8)
    lane = lax.broadcasted_iota(jnp.int32, (TOK_DEV, 128), 1)
    low_half = lane % HD < HD // 2
    left = lane < HD
    for tile in range(HEADS // 2):
        raw = q_ref[:, tile * 128 : (tile + 1) * 128].astype(jnp.float32)
        turned = jnp.where(low_half, pltpu.roll(raw, 128 - HD // 2, 1), pltpu.roll(raw, HD // 2, 1))
        rotated = raw * cos_ref[...] + turned * sin_ref[...]
        rotated = rotated.astype(jnp.bfloat16).astype(jnp.float32) * (HD**-0.5)
        swapped_halves = pltpu.roll(rotated, HD, 1)
        for odd in (0, 1):
            head = tile * 2 + odd
            group, member = head // GROUP, head % GROUP
            want_left = group % 2 == 0
            source = rotated if (odd == 0) == want_left else swapped_halves
            kept = jnp.where(left == want_left, source, 0.0).astype(jnp.bfloat16)
            for part in (0, 1):
                q_sc[part, group, member * HALF : (member + 1) * HALF, :] = kept[
                    part * HALF : (part + 1) * HALF
                ]
                max_sc[part, group, member * HALF : (member + 1) * HALF, :] = jnp.full(
                    (HALF, 128), sink_ref[head], jnp.float32
                )
    wide = GROUP * HALF
    acc_left = lax.broadcasted_iota(jnp.int32, (wide, 128), 1) < HD
    for part in (0, 1):
        for group in range(KVH):
            acc_sc[part, group] = jnp.where(acc_left == (group % 2 == 0), 0.0, 1.0)
    v_left = lax.broadcasted_iota(jnp.int32, (BLOCK, 128), 1) < HD
    row_in_span = lax.broadcasted_iota(jnp.int32, (wide, BLOCK), 0) % HALF
    key_in_block = lax.broadcasted_iota(jnp.int32, (wide, BLOCK), 1)

    def unit(part, block, first_query):
        at = pl.multiple_of(block * BLOCK, BLOCK)
        for group in range(KVH):
            tile = group // 2
            key_tile = keys[pl.ds(at, BLOCK), tile * 128 : (tile + 1) * 128]
            value_tile = keys[pl.ds(at, BLOCK), KVH * HD + tile * 128 : KVH * HD + (tile + 1) * 128]
            value_tile = jnp.where(
                v_left == (group % 2 == 0), value_tile, jnp.ones_like(value_tile)
            )
            scores = lax.dot_general(
                q_sc[part, group],
                key_tile,
                (((1,), (1,)), ((), ())),
                preferred_element_type=jnp.float32,
            )
            if first_query is not None:
                scores = jnp.where(
                    key_in_block + at <= row_in_span + first_query, scores, masked_score
                )
            old_max = max_sc[part, group]
            new_max = jnp.maximum(old_max, jnp.max(scores, axis=1, keepdims=True))
            weights = jnp.exp(scores - new_max[:, :1])
            added = jnp.dot(
                weights.astype(jnp.bfloat16), value_tile, preferred_element_type=jnp.float32
            )
            max_sc[part, group] = new_max
            acc_sc[part, group] = acc_sc[part, group] * jnp.exp(old_max - new_max) + added

    per_block = BLOCK // HALF
    for part in (0, 1):
        span = order_ref[2 * seq + part]
        full = span // per_block

        def body(block, carry, part=part):
            unit(part, block, None)
            return carry

        lax.fori_loop(0, full, body, 0)
        unit(part, full, span * HALF)
    for part in (0, 1):
        for group in range(KVH):
            total = acc_sc[part, group]
            divided = total / pltpu.roll(total, HD, 1)
            for pair in range(GROUP // 2):
                one = divided[2 * pair * HALF : (2 * pair + 1) * HALF]
                two = divided[(2 * pair + 1) * HALF : (2 * pair + 2) * HALF]
                if group % 2 == 0:
                    two = pltpu.roll(two, HD, 1)
                else:
                    one = pltpu.roll(one, HD, 1)
                tile = group * (GROUP // 2) + pair
                rows[part * HALF : (part + 1) * HALF, tile * 128 : (tile + 1) * 128] = jnp.where(
                    left[:HALF], one, two
                ).astype(jnp.bfloat16)


def attend(span_order, sinks, queries, cos, sin, kv_all):
    spec = pl.BlockSpec(memory_space=pltpu.VMEM)
    smem = pl.BlockSpec(memory_space=pltpu.SMEM)
    wide = GROUP * HALF
    return pl.pallas_call(
        attention_kernel,
        out_shape=jax.ShapeDtypeStruct(queries.shape, jnp.bfloat16),
        in_specs=[smem, smem] + [spec] * 4,
        out_specs=spec,
        scratch_shapes=[
            pltpu.VMEM(kv_all.shape, jnp.bfloat16),
            pltpu.VMEM((2, KVH, wide, 128), jnp.bfloat16),
            pltpu.VMEM((2, KVH, wide, 128), jnp.float32),
            pltpu.VMEM((2, KVH, wide, 128), jnp.float32),
        ],
        compiler_params=pltpu.CompilerParams(vmem_limit_bytes=30 * 1024 * 1024),
        cost_estimate=pl.CostEstimate(
            flops=4_000_000_000, bytes_accessed=8_000_000, transcendentals=5_000_000
        ),
        name="attend",
    )(span_order, sinks, queries, cos, sin, kv_all)


def on_device(
    residual,
    queries,
    key_rows,
    values,
    attention_sinks,
    out_weight,
    norm_gain,
    router_weight,
    gate_weight,
    up_weight,
    down_weight,
    routing,
    span_order,
):
    seq_count = lax.axis_size("seq")
    token_count = residual.shape[1]
    own = (gate_weight, up_weight, down_weight)
    rings = seq_count // 4
    kv_all, w_all, cos, sin, *other = gather_all(
        span_order, key_rows[0], values[0], out_weight, own, rings
    )
    rows = attend(
        span_order,
        attention_sinks,
        queries[0],
        cos,
        sin,
        kv_all.reshape(seq_count * token_count, 2 * KVH * HD),
    )
    attended, layer_output = moe(
        rings,
        2,
        rows,
        w_all,
        residual[0],
        norm_gain[None, :],
        router_weight.T,
        routing[0].T,
        own,
        other,
    )
    return (attended[None], layer_output[None])


def solution(mesh):
    in_specs = (
        P("fsdp", "seq", None),
        P("fsdp", "seq", None),
        P("fsdp", "seq", None),
        P("fsdp", "seq", None),
        P(),
        P("seq", "fsdp"),
        P(),
        P(),
        P(None, "seq"),
        P(None, "seq"),
        P("seq", None),
        P("fsdp", "seq", None),
        P(),
    )
    out_specs = (P("fsdp", "seq", None), P("fsdp", "seq", None))
    return jax.shard_map(
        on_device, mesh=mesh, in_specs=in_specs, out_specs=out_specs, check_vma=False
    )
```
